32 devices in a mesh: seq: 16 (over z, y, x), head: 2 (over core).
Axes of the slice: x: 2, y: 2, z: 4, core: 2. Of those that a mesh axis runs over, the one named last changes fastest.
Arguments:
- tokens: bfloat16 [8192, 3584], P('seq', 'head'), may hold values from -6 to 6
- pre_gain: float32 [3584], replicated, may hold values from 0.5 to 1.5
- query_weight: bfloat16 [3584, 2048], P(None, 'head'), may hold values from -0.375 to 0.375
- key_weight: bfloat16 [3584, 1024], P(None, 'head'), may hold values from -0.375 to 0.375
- value_weight: bfloat16 [3584, 1024], P(None, 'head'), may hold values from -0.09375 to 0.09375
- out_weight: bfloat16 [2048, 3584], P('head'), may hold values from -0.5 to 0.5
- post_gain: float32 [3584], P('head'), may hold values from 0.5 to 1.5
Outputs:
- layer_out: bfloat16 [8192, 3584], P('seq', 'head')
The draws below stay inside these ranges and needn't reach their ends.
All inputs are finite; a program needn't handle non-finite values.
Results may differ from the reference program's by a relative error of at most 0.013.
The reference program's roundings to bfloat16 on the way count: a program that leaves them out, or rounds other values in their place, can miss the bound.
Values may be sent and summed in bfloat16 or wider, within the bound.
A program may use at most 192 MiB of HBM per device.

```python
import jax
import jax.numpy as jnp
from jax import lax

D = 3584
QH = 8
KVH = 4
HD = 256
WINDOW = 4096
TOK_DEV = 512
TOKENS = 8192


def draw_out_weight(key, part):
    key_entries = jax.random.fold_in(key, 11)
    key_columns = jax.random.fold_in(key, 12)
    fan_in = QH * HD
    ramp = 3.0 ** (jnp.arange(D, dtype=jnp.float32) / D)
    column_scale = jnp.exp(jax.random.uniform(key_columns, (D,), jnp.float32) * jnp.log(10.0)) * ramp / 6.0
    entries = jax.random.truncated_normal(key_entries, -4.0, 4.0, (fan_in, D), jnp.float32)
    matrix = entries * column_scale[None, :] * (fan_in * 1.0) ** (-0.5)
    return jnp.clip(matrix, -0.5, 0.5).astype(jnp.bfloat16)


def block_scale(stream_key, shape, split, smallest, high):
    level = 1.0
    for dim, shards_of in split:
        steps = jax.random.uniform(jax.random.fold_in(jax.random.fold_in(stream_key, 6), dim), (shards_of,), jnp.float32, smallest / len(split), high / len(split))
        level = level * jnp.repeat(jnp.exp(steps), shape[dim] // shards_of).reshape((-1,) + (1,) * (len(shape) - 1 - dim))
    return level


def scatter_about(rng, shape, width, limit, pieces=(), held_as=jnp.bfloat16):
    drawn = width * jax.random.normal(rng, shape, jnp.float32)
    if pieces:
        drawn = drawn * block_scale(rng, shape, pieces, -0.22, 0.18)
    return jnp.clip(drawn, -limit, limit).astype(held_as)


def setup_inputs(seed: int = 0) -> dict:
    streams_of = jax.random.split(jax.random.key(seed), 8)
    return {
        "tokens": scatter_about(streams_of[0], (TOKENS, D), 1.0, 6.0, ((0, 16), (1, 2))),
        "pre_gain": jnp.clip(1.0 + 0.1 * jax.random.normal(streams_of[1], (D,), jnp.float32), 0.5, 1.5),
        "query_weight": scatter_about(streams_of[2], (D, QH * HD), (D // 16) ** -0.5, 0.375, ((1, 2),)),
        "key_weight": scatter_about(streams_of[3], (D, KVH * HD), (D // 16) ** -0.5, 0.375, ((1, 2),)),
        "value_weight": scatter_about(streams_of[4], (D, KVH * HD), D ** -0.5, 0.09375, ((1, 2),)),
        "out_weight": draw_out_weight(jax.random.fold_in(streams_of[7], 71), 0),
        "post_gain": jnp.clip(1.0 + 0.1 * jax.random.normal(streams_of[6], (D,), jnp.float32), 0.5, 1.5),
    }


softcap_limit = 50.0
rope_base = 10000.0
norm_epsilon = 1e-06

def rms_scale(values):
    return lax.rsqrt(lax.optimization_barrier(jnp.sum(values * values, axis=-1, keepdims=True)) / values.shape[-1] + norm_epsilon)

def rotate(values, positions):
    midpoint = values.shape[-1] // 2
    frequency = jnp.exp(-jnp.log(rope_base) * (2.0 * jnp.arange(midpoint, dtype=jnp.float32) / values.shape[-1]))
    angles = positions.astype(jnp.float32)[:, None] * frequency[None, :]
    cosine = jnp.cos(angles)[:, None, :]
    sine_part = jnp.sin(angles)[:, None, :]
    leading = values[..., :midpoint]
    trailing = values[..., midpoint:]
    return jnp.concatenate([leading * cosine - trailing * sine_part, trailing * cosine + leading * sine_part], axis=-1)

def reference(tokens, pre_gain, query_weight, key_weight, value_weight, out_weight, post_gain):
    widened = tokens.astype(jnp.float32)
    normed = (widened * rms_scale(widened) * pre_gain).astype(jnp.bfloat16)
    positions = jnp.arange(TOKENS, dtype=jnp.int32)
    queries = rotate(jnp.dot(normed, query_weight, preferred_element_type=jnp.float32).reshape(TOKENS, QH, HD), positions).astype(jnp.bfloat16)
    keys_all = rotate(jnp.dot(normed, key_weight, preferred_element_type=jnp.float32).reshape(TOKENS, KVH, HD), positions).astype(jnp.bfloat16)
    values_all = jnp.dot(normed, value_weight, preferred_element_type=jnp.float32).reshape(TOKENS, KVH, HD).astype(jnp.bfloat16)
    queries = lax.optimization_barrier(queries).astype(jnp.float32)
    keys_all = lax.optimization_barrier(keys_all).astype(jnp.float32)
    values_all = lax.optimization_barrier(values_all).astype(jnp.float32)
    group_size = QH // KVH
    padding = jnp.zeros((WINDOW, KVH, HD), jnp.float32)
    keys_padded = jnp.concatenate([padding, keys_all], axis=0)
    values_padded = jnp.concatenate([padding, values_all], axis=0)

    def one_block(block_index):
        first_row = block_index * TOK_DEV
        query_block = lax.dynamic_slice_in_dim(queries, first_row, TOK_DEV, 0).reshape(TOK_DEV, KVH, group_size, HD)
        key_block = lax.dynamic_slice_in_dim(keys_padded, first_row, WINDOW + TOK_DEV, 0)
        value_block = lax.dynamic_slice_in_dim(values_padded, first_row, WINDOW + TOK_DEV, 0)
        query_index = first_row + jnp.arange(TOK_DEV, dtype=jnp.int32)
        key_index = first_row - WINDOW + jnp.arange(WINDOW + TOK_DEV, dtype=jnp.int32)
        scores = jnp.einsum('qkgd,skd->kgqs', query_block, key_block) * HD ** (-0.5)
        capped = softcap_limit * jnp.tanh(scores / softcap_limit)
        offset = query_index[:, None] - key_index[None, :]
        allowed = (offset >= 0) & (offset < WINDOW) & (key_index[None, :] >= 0)
        weights = jnp.where(allowed, jnp.exp(capped), 0.0)
        denominator = lax.optimization_barrier(jnp.sum(weights, axis=-1))
        rounded = lax.optimization_barrier(weights.astype(jnp.bfloat16)).astype(jnp.float32)
        numerator = jnp.einsum('kgqs,skd->qkgd', rounded, value_block)
        attended_block = numerator / jnp.transpose(denominator, (2, 0, 1))[..., None]
        return attended_block.astype(jnp.bfloat16).reshape(TOK_DEV, QH * HD)
    attended = lax.map(one_block, jnp.arange(TOKENS // TOK_DEV, dtype=jnp.int32)).reshape(TOKENS, QH * HD)
    branch = jnp.dot(attended, out_weight, preferred_element_type=jnp.float32)
    return (widened + post_gain * branch * rms_scale(branch)).astype(jnp.bfloat16)
```

```python
import functools
import math

import jax
import jax.numpy as jnp
import numpy as np
from jax import lax
from jax.experimental import pallas as pl
from jax.experimental.pallas import tpu as pltpu
from jax.sharding import PartitionSpec as P

HD = 256
LANES = 128
WINDOW = 4096

softcap_limit = 50.0
rope_base = 10000.0
norm_epsilon = 1e-06

CHUNKS = 4
UNITS = 2

TOKEN = 0
X_KV = TOKEN + CHUNKS
X_Q = X_KV + CHUNKS
X_OUT = X_Q + 1
Z_NEAR = X_OUT + CHUNKS
Z_FAR = Z_NEAR + 2 * CHUNKS
Y_NEAR = Z_FAR + 2 * CHUNKS
Y_FAR = Y_NEAR + 2 * CHUNKS
GIVEN = Y_FAR + 2 * CHUNKS
SQUARES = GIVEN + CHUNKS
MESSAGES = SQUARES + CHUNKS

L_TOKEN = 0
L_GAIN = L_TOKEN + CHUNKS
L_FREQ = L_GAIN + 1
L_POST = L_FREQ + 1
L_KV = L_POST + 1
L_Q = L_KV + 8
L_OUT = L_Q + 4
LOCALS = L_OUT + 4

inner = 1.0 / (math.sqrt(HD) * softcap_limit)
outer = softcap_limit / math.log(2.0)


def rotated(head, cosine, sine):
    midpoint = HD // 2
    leading, trailing = head[:, :midpoint], head[:, midpoint:]
    return jnp.concatenate(
        [leading * cosine - trailing * sine, trailing * cosine + leading * sine], axis=-1
    ).astype(jnp.bfloat16)


def layer_kernel(
    blocks, tokens_hbm, gain_hbm, freq_hbm, wq_hbm, wk_hbm, wv_hbm, wo_hbm, post_hbm, out_ref,
    own, other, gain, freq, post, normed, wkv, wq, wo, cosine, sine, held, kvm, queries, asked,
    total, mass, leaving, landed, finished, branch, given, arrived, sq_own, sq_other,
    send_sems, recv_sems, local_sems,
):
    rows, width = own.shape
    part = rows // CHUNKS
    unit = rows // UNITS
    group = 2 * 2
    me = lax.axis_index("seq")
    side = lax.axis_index("head")
    x = me % 2
    y = (me // 2) % 2
    x_mate = me + 1 - 2 * x
    y_mate = me + 2 - 4 * y
    z_next = me + group
    has_next = z_next < blocks
    has_prev = me >= group
    has_far = me >= 2 * group
    first_row = y == 0
    second_row = y == 1

    def local(index, src, dst):
        return pltpu.make_async_copy(src, dst, local_sems.at[index])

    def copy(message, src, dst, device):
        return pltpu.make_async_remote_copy(
            src_ref=src,
            dst_ref=dst,
            send_sem=send_sems.at[message],
            recv_sem=recv_sems.at[message],
            device_id=device,
            device_id_type=pl.DeviceIdType.MESH,
        )

    to_x = {"seq": x_mate}
    to_y = {"seq": y_mate}
    to_z = {"seq": z_next}
    to_core = {"head": 1 - side}

    def chunk(p):
        return pl.ds(pl.multiple_of(p * part, part), part)

    halves = (side, 1 - side)
    pairs = (x, 1 - x)

    own_copy = [local(L_TOKEN + p, tokens_hbm.at[chunk(p)], own.at[chunk(p)]) for p in range(CHUNKS)]
    gain_copy = local(L_GAIN, gain_hbm, gain)
    freq_copy = local(L_FREQ, freq_hbm, freq)
    post_copy = local(L_POST, post_hbm, post)
    kv_copies = [[], []]
    q_copies = [[], []]
    out_copies = [[], []]
    for i in range(2):
        for f in range(2):
            at_rows = pl.ds(pl.multiple_of(halves[f] * width, width), width)
            for n, source in enumerate((wk_hbm, wv_hbm)):
                columns = pl.ds(pl.multiple_of(pairs[i] * HD, HD), HD)
                kv_copies[i].append(
                    local(
                        L_KV + 4 * i + 2 * f + n,
                        source.at[at_rows, columns],
                        wkv.at[i, pl.ds(f * width, width), pl.ds(n * HD, HD)],
                    )
                )
            columns = pl.ds(pl.multiple_of(pairs[i] * 2 * HD, 2 * HD), 2 * HD)
            q_copies[i].append(
                local(
                    L_Q + 2 * i + f,
                    wq_hbm.at[at_rows, columns],
                    wq.at[i, pl.ds(f * width, width), :],
                )
            )
            at_heads = pl.ds(pl.multiple_of(pairs[i] * 2 * HD, 2 * HD), 2 * HD)
            columns = pl.ds(pl.multiple_of(halves[1 - f] * width, width), width)
            out_copies[i].append(local(L_OUT + 2 * i + f, wo_hbm.at[at_heads, columns], wo.at[i, f]))

    order = [CHUNKS - 1 - i for i in range(CHUNKS)]
    for p in order:
        own_copy[p].start()
    freq_copy.start()
    gain_copy.start()
    for c in kv_copies[0]:
        c.start()

    barrier = pltpu.get_barrier_semaphore()

    def greet(device):
        pl.semaphore_signal(barrier, inc=1, device_id=device, device_id_type=pl.DeviceIdType.MESH)

    greet(to_core)
    greet(to_x)
    greet(to_y)
    pl.when(has_next)(lambda: greet(to_z))
    pl.when(has_prev)(lambda: greet({"seq": me - group}))
    pl.semaphore_wait(barrier, 3 + has_next.astype(jnp.int32) + has_prev.astype(jnp.int32))

    def token_copy(p):
        return copy(TOKEN + p, tokens_hbm.at[chunk(p)], other.at[chunk(p)], to_core)

    for p in order:
        token_copy(p).start()
    for c in kv_copies[1]:
        c.start()
    for i in (1, 0):
        for c in q_copies[i]:
            c.start()

    def piece(ref, p):
        return ref.at[:, chunk(p), :]

    def of(r):
        return x + r - 2 * x * r

    def send_x(p):
        return copy(X_KV + p, piece(kvm, p), piece(held.at[0, x], p), to_x)

    def take_x(p):
        return copy(X_KV + p, piece(kvm, p), piece(held.at[0, 1 - x], p), to_x)

    def place(r, p):
        return r * CHUNKS + CHUNKS - 1 - p

    def z_near(r, p):
        b = of(r)
        return copy(Z_NEAR + place(r, p), piece(held.at[0, b], p), piece(held.at[2, b], p), to_z)

    def z_far(b, p):
        return copy(Z_FAR + place(1 - b, p), piece(held.at[2, b], p), piece(held.at[4, b], p), to_z)

    def y_near(slot, r, p):
        b = of(r)
        return copy(Y_NEAR + place(r, p), piece(held.at[slot, b], p), piece(held.at[1, b], p), to_y)

    def y_far(slot, b, p):
        return copy(Y_FAR + place(1 - b, p), piece(held.at[slot, b], p), piece(held.at[3, b], p), to_y)

    freq_copy.wait()
    at_row = lax.broadcasted_iota(jnp.int32, (rows, LANES), 0) + me * rows
    angles = at_row.astype(jnp.float32) * freq[...]
    cosine[...] = jnp.cos(angles)
    sine[...] = jnp.sin(angles)
    total[...] = jnp.zeros_like(total)
    mass[...] = jnp.zeros_like(mass)
    gain_copy.wait()

    lines = 16
    tiles = width // LANES

    def norm_chunk(p):
        def step(i, carry):
            at = pl.ds(pl.multiple_of(p * part + i * lines, lines), lines)
            squares = None
            for ref in (own, other):
                for j in range(tiles):
                    value = ref[at, j * LANES : (j + 1) * LANES].astype(jnp.float32)
                    squares = value * value if squares is None else squares + value * value
            scale = lax.rsqrt(
                jnp.sum(squares, axis=-1, keepdims=True) / (2 * width) + norm_epsilon
            )
            scale = jnp.broadcast_to(scale, (lines, LANES))
            for f, ref in enumerate((own, other)):
                for j in range(tiles):
                    value = ref[at, j * LANES : (j + 1) * LANES].astype(jnp.float32)
                    weight = gain[pl.ds(halves[f] * tiles + j, 1), :]
                    to = f * width + j * LANES
                    normed[at, to : to + LANES] = (value * scale * weight).astype(jnp.bfloat16)
            return carry

        lax.fori_loop(0, part // lines, step, 0)

    def project_kv(p, i, dst):
        value = jnp.dot(normed[chunk(p), :], wkv[i], preferred_element_type=jnp.float32)
        key = rotated(value[:, :HD], cosine[chunk(p), :], sine[chunk(p), :])
        dst[0, chunk(p), :] = key
        dst[1, chunk(p), :] = value[:, HD:].astype(jnp.bfloat16)

    def take_near(r, p):
        def act():
            z_near(r, p).wait_recv()
            pl.when(second_row)(lambda: y_near(2, r, p).start())

        pl.when(has_prev)(act)

    def pass_far(b, p):
        def act():
            pl.when(has_next)(lambda: z_far(b, p).start())
            pl.when(first_row)(lambda: y_far(2, b, p).start())

        pl.when(has_prev)(act)

    def take_far(b, p):
        def act():
            z_far(b, p).wait_recv()
            pl.when(second_row)(lambda: y_far(4, b, p).start())

        pl.when(has_far)(act)

    def pass_mate(p):
        take_x(p).wait_recv()
        pl.when(has_next)(lambda: z_near(1, p).start())
        pl.when(first_row)(lambda: y_near(0, 1, p).start())

    for i, p in enumerate(order):
        own_copy[p].wait()
        token_copy(p).wait_recv()
        norm_chunk(p)
        if i == 0:
            for c in kv_copies[0]:
                c.wait()
        project_kv(p, 0, held.at[0, x])
        pl.when(has_next)(lambda: z_near(0, p).start())
        pl.when(first_row)(lambda: y_near(0, 0, p).start())
        if i == 0:
            for c in kv_copies[1]:
                c.wait()
        project_kv(p, 1, kvm)
        send_x(p).start()
        if i == 0:
            for i_ in (0, 1):
                for c in out_copies[i_]:
                    c.start()
            post_copy.start()
        if i == 2:
            take_near(0, order[0])

    def project_q(i, dst):
        def step(t, carry):
            at = pl.ds(pl.multiple_of(t * unit, unit), unit)
            value = jnp.dot(normed[at, :], wq[i], preferred_element_type=jnp.float32)
            for head in range(2):
                dst[pl.ds(pl.multiple_of(head * rows + t * unit, unit), unit), :] = rotated(
                    value[:, head * HD : (head + 1) * HD], cosine[at, :], sine[at, :]
                )
            return carry

        lax.fori_loop(0, UNITS, step, 0)

    def q_copy():
        return copy(X_Q, asked, queries.at[1], to_x)

    pass_mate(order[0])
    for c in q_copies[1]:
        c.wait()
    take_near(0, order[1])
    project_q(1, asked)
    q_copy().start()
    pass_mate(order[1])
    take_near(0, order[2])
    for c in q_copies[0]:
        c.wait()
    project_q(0, queries.at[0])
    pass_mate(order[2])
    take_near(0, order[3])
    pass_mate(order[3])

    def attend(which, slot, b, h, distance=None):
        at = pl.ds(pl.multiple_of(h * unit, unit), unit)
        scores = lax.dot_general(
            queries[which],
            held[slot, b, 0, at, :],
            (((1,), (1,)), ((), ())),
            preferred_element_type=jnp.float32,
        )
        weights = jnp.exp2(outer * jnp.tanh(scores * inner))
        if distance is not None:
            down = lax.broadcasted_iota(jnp.int32, weights.shape, 0)
            down = jnp.where(down >= rows, down - rows, down)
            offset = (distance - h * unit) + down - lax.broadcasted_iota(jnp.int32, weights.shape, 1)
            weights = jnp.where((offset >= 0) & (offset < WINDOW), weights, 0.0)
        added = None
        for k in range(unit // LANES):
            lanes = weights[:, k * LANES : (k + 1) * LANES]
            added = lanes if added is None else added + lanes
        mass[which] += added
        total[which] += jnp.dot(
            weights.astype(jnp.bfloat16), held[slot, b, 1, at, :], preferred_element_type=jnp.float32
        )

    def both(act):
        def step(s, carry):
            act(s)
            return carry

        lax.fori_loop(0, 2, step, 0)

    def attend_own(which):
        mine = of(which)

        def step(i, carry):
            b = mine - i // UNITS
            attend(which, 0, b, i % UNITS, (mine - b) * rows)
            return carry

        lax.fori_loop(0, UNITS + UNITS * mine, step, 0)

    def z_unit(u):
        return 2, of(u // UNITS), UNITS - 1 - u % UNITS

    def y_unit(w):
        far = w // 4
        r = (w % 4) // UNITS
        b = (1 - far) * of(r) + far * (1 - r)
        return 1 + 2 * far, b, UNITS - 1 - w % UNITS

    def y_there(w):
        return me >= 2 + 4 * (w // 4)

    def take_y(w):
        slot, b, h = y_unit(w)
        for n in range(CHUNKS // UNITS):
            k = CHUNKS // UNITS * w + n
            p = CHUNKS - 1 - k % CHUNKS
            copy(Y_NEAR + k, piece(held.at[slot, b], p), piece(held.at[slot, b], p), to_y).wait_recv()

    attend_own(0)

    def near_step(u, carry):
        p = CHUNKS - 1 - u
        take_near(1, p)
        pass_far(1, p)
        pl.when(has_prev)(lambda: attend(0, *z_unit(u)))

        def with_y():
            take_y(u - 1)
            attend(0, *y_unit(u - 1))

        pl.when((u >= 1) & y_there(0))(with_y)
        return carry

    lax.fori_loop(0, 4, near_step, 0)
    for p in order:
        pass_far(0, p)

    q_copy().wait_recv()
    attend_own(1)
    take_far(1, order[0])

    def again_z(u, carry):
        attend(1, *z_unit(u))
        return carry

    def repeat(count, step):
        def act():
            lax.fori_loop(0, count, step, 0)

        return act

    pl.when(has_prev)(repeat(4, again_z))
    take_far(1, order[1])

    def again_y(w, carry):
        attend(1, *y_unit(w))
        return carry

    pl.when(y_there(0))(repeat(3, again_y))

    def whole_y(w):
        def act():
            take_y(w)
            both(lambda s: attend(s, *y_unit(w)))

        pl.when(y_there(w))(act)

    def take_next(k):
        def act():
            take_far(1 - k // CHUNKS, CHUNKS - 1 - k % CHUNKS)

        pl.when(k < 2 * CHUNKS)(act)

    def far_step(v, carry):
        whole_y(3 + v)
        take_next(2 + 2 * v)

        def far_unit():
            b = 1 - v // UNITS

            def one(s):
                mine = of(s)
                pl.when(mine <= b)(
                    lambda: attend(s, 4, b, UNITS - 1 - v % UNITS, WINDOW + (mine - b) * rows)
                )

            both(one)

        pl.when(has_far)(far_unit)
        take_next(3 + 2 * v)
        return carry

    lax.fori_loop(0, 4, far_step, 0)
    whole_y(7)

    def finish(which, head, at_rows):
        at = pl.ds(head * rows + at_rows.start, at_rows.size)
        weight = jnp.sum(mass[which, at, :], axis=-1, keepdims=True)
        return (total[which, at, :] * (1.0 / weight)).astype(jnp.bfloat16)

    def out_copy(p):
        return copy(X_OUT + p, leaving.at[chunk(p)], landed.at[chunk(p)], to_x)

    for p in range(CHUNKS):
        for head in range(2):
            leaving[chunk(p), head * HD : (head + 1) * HD] = finish(1, head, chunk(p))
        out_copy(p).start()
    for p in range(CHUNKS):
        for head in range(2):
            finished[chunk(p), head * HD : (head + 1) * HD] = finish(0, head, chunk(p))
    for i in (0, 1):
        for c in out_copies[i]:
            c.wait()
    post_copy.wait()

    for f in range(2):
        def column(t, carry):
            at = pl.ds(pl.multiple_of(t * HD, HD), HD)
            branch[f, :, at] = jnp.dot(
                finished[...], wo[0, f, :, at], preferred_element_type=jnp.float32
            )
            return carry

        lax.fori_loop(0, width // HD, column, 0)

    def given_copy(p):
        return copy(GIVEN + p, given.at[chunk(p)], arrived.at[chunk(p)], to_core)

    def squares_copy(p):
        return copy(SQUARES + p, sq_own.at[chunk(p)], sq_other.at[chunk(p)], to_core)

    def add_mate(p):
        out_copy(p).wait_recv()
        theirs = landed[chunk(p), :]
        given[chunk(p), :] = (
            branch[0, chunk(p), :]
            + jnp.dot(theirs, wo[1, 0], preferred_element_type=jnp.float32)
        ).astype(jnp.bfloat16)
        given_copy(p).start()
        branch[1, chunk(p), :] += jnp.dot(theirs, wo[1, 1], preferred_element_type=jnp.float32)

    def add_core(p):
        given_copy(p).wait_recv()
        squares = None
        for j in range(tiles):
            at = slice(j * LANES, (j + 1) * LANES)
            share = branch[1, chunk(p), at] + arrived[chunk(p), at].astype(jnp.float32)
            branch[1, chunk(p), at] = share
            squares = share * share if squares is None else squares + share * share
        sq_own[chunk(p), :] = squares
        squares_copy(p).start()

    def last(p):
        squares_copy(p).wait_recv()
        squares = jnp.sum(sq_own[chunk(p), :] + sq_other[chunk(p), :], axis=-1, keepdims=True)
        scale = jnp.broadcast_to(
            lax.rsqrt(squares / (2 * width) + norm_epsilon), (part, LANES)
        )
        for j in range(tiles):
            at = slice(j * LANES, (j + 1) * LANES)
            out_ref[chunk(p), at] = (
                own[chunk(p), at].astype(jnp.float32)
                + post[j : j + 1, :] * branch[1, chunk(p), at] * scale
            ).astype(jnp.bfloat16)

    def tail(p, carry):
        pl.when(p < CHUNKS)(lambda: add_mate(p))
        pl.when((p >= 1) & (p < CHUNKS + 1))(lambda: add_core(p - 1))
        pl.when(p >= 2)(lambda: last(p - 2))
        return carry

    lax.fori_loop(0, CHUNKS + 2, tail, 0)

    q_copy().wait_send()
    for p in order:
        token_copy(p).wait_send()
        send_x(p).wait_send()
        out_copy(p).wait_send()
        given_copy(p).wait_send()
        squares_copy(p).wait_send()
    for r in range(2):
        for p in order:
            pl.when(has_next)(lambda: z_near(r, p).wait_send())
            pl.when(has_next & has_prev)(lambda: z_far(r, p).wait_send())
            pl.when(first_row)(lambda: y_near(0, r, p).wait_send())
            pl.when(first_row & has_prev)(lambda: y_far(2, r, p).wait_send())
            pl.when(second_row & has_prev)(lambda: y_near(2, r, p).wait_send())
            pl.when(second_row & has_far)(lambda: y_far(4, r, p).wait_send())


def local_layer(blocks, tokens, pre_gain, query_weight, key_weight, value_weight, out_weight, post_gain):
    rows, width = tokens.shape
    frequency = np.exp(-np.log(rope_base) * (2.0 * np.arange(HD // 2) / HD)).astype(np.float32)
    anywhere = pl.BlockSpec(memory_space=pl.ANY)
    bf16, f32 = jnp.bfloat16, jnp.float32
    vmem = pltpu.VMEM
    half = 2 * HD
    return pl.pallas_call(
        functools.partial(layer_kernel, blocks),
        out_shape=jax.ShapeDtypeStruct((rows, width), bf16),
        in_specs=[anywhere] * 8,
        out_specs=pl.BlockSpec(memory_space=pltpu.VMEM),
        scratch_shapes=[
            vmem((rows, width), bf16),
            vmem((rows, width), bf16),
            vmem((2 * width // LANES, LANES), f32),
            vmem((1, LANES), f32),
            vmem((width // LANES, LANES), f32),
            vmem((rows, 2 * width), bf16),
            vmem((2, 2 * width, half), bf16),
            vmem((2, 2 * width, half), bf16),
            vmem((2, 2, half, width), bf16),
            vmem((rows, LANES), f32),
            vmem((rows, LANES), f32),
            vmem((5, 2, 2, rows, HD), bf16),
            vmem((2, rows, HD), bf16),
            vmem((2, 2 * rows, HD), bf16),
            vmem((2 * rows, HD), bf16),
            vmem((2, 2 * rows, HD), f32),
            vmem((2, 2 * rows, LANES), f32),
            vmem((rows, half), bf16),
            vmem((rows, half), bf16),
            vmem((rows, half), bf16),
            vmem((2, rows, width), f32),
            vmem((rows, width), bf16),
            vmem((rows, width), bf16),
            vmem((rows, LANES), f32),
            vmem((rows, LANES), f32),
            pltpu.SemaphoreType.DMA((MESSAGES,)),
            pltpu.SemaphoreType.DMA((MESSAGES,)),
            pltpu.SemaphoreType.DMA((LOCALS,)),
        ],
        compiler_params=pltpu.CompilerParams(
            collective_id=0, has_side_effects=True, vmem_limit_bytes=62 * 1024 * 1024
        ),
    )(
        tokens,
        pre_gain.reshape(-1, LANES),
        jnp.asarray(frequency)[None, :],
        query_weight,
        key_weight,
        value_weight,
        out_weight,
        post_gain.reshape(-1, LANES),
    )


def solution(mesh):
    placed = (
        P("seq", "head"),
        P(),
        P(None, "head"),
        P(None, "head"),
        P(None, "head"),
        P("head", None),
        P("head"),
    )
    return jax.shard_map(
        functools.partial(local_layer, mesh.shape["seq"]),
        mesh=mesh,
        in_specs=placed,
        out_specs=P("seq", "head"),
        check_vma=False,
    )
```

```python
import functools
import math

import jax
import jax.numpy as jnp
import numpy as np
from jax import lax
from jax.experimental import pallas as pl
from jax.experimental.pallas import tpu as pltpu
from jax.sharding import PartitionSpec as P

HD = 256
LANES = 128
WINDOW = 4096

softcap_limit = 50.0
rope_base = 10000.0
norm_epsilon = 1e-06

CHUNKS = 4
UNITS = 2

TOKEN = 0
X_KV = TOKEN + CHUNKS
X_Q = X_KV + CHUNKS
X_OUT = X_Q + 1
Z_NEAR = X_OUT + CHUNKS
Z_FAR = Z_NEAR + 2 * CHUNKS
Z_EXTRA = Z_FAR + CHUNKS + CHUNKS // 2
Y_NEAR = Z_EXTRA + CHUNKS // 2
Y_FAR = Y_NEAR + 2 * UNITS
Y_EXTRA = Y_FAR + 2 * UNITS
GIVEN = Y_EXTRA + 1
SQUARES = GIVEN + CHUNKS
MESSAGES = SQUARES + CHUNKS

(
    S_TOKEN, S_X, S_Q, S_OUT, S_Z_NEAR, S_Z_FAR, S_Y_NEAR, S_Y_FAR, S_Y_LATE, S_Y_EXTRA, S_GIVEN,
    S_SQUARES, SENDS,
) = range(13)

L_TOKEN = 0
L_GAIN = L_TOKEN + CHUNKS
L_FREQ = L_GAIN + 1
L_POST = L_FREQ + 1
L_KV = L_POST + 1
L_Q = L_KV + 2
L_OUT = L_Q + 2
LOCALS = L_OUT + 1

inner = 1.0 / (math.sqrt(HD) * softcap_limit)
outer = softcap_limit / math.log(2.0)


def rotated(head, cosine, sine):
    midpoint = HD // 2
    leading, trailing = head[:, :midpoint], head[:, midpoint:]
    return jnp.concatenate(
        [leading * cosine - trailing * sine, trailing * cosine + leading * sine], axis=-1
    ).astype(jnp.bfloat16)


def layer_kernel(
    blocks, tokens_hbm, gain_hbm, freq_hbm, wq_hbm, wk_hbm, wv_hbm, wo_hbm, post_hbm, out_ref,
    own, other, gain, freq, post, normed, wkv, wq, wo, cosine, sine, held, kvm, queries, asked,
    total, mass, leaving, landed, finished, branch, arrived, sq_own, sq_other,
    send_sems, recv_sems, local_sems,
):
    rows, width = own.shape
    part = rows // CHUNKS
    unit = rows // UNITS
    group = 2 * 2
    me = lax.axis_index("seq")
    side = lax.axis_index("head")
    x = me % 2
    y = (me // 2) % 2
    x_mate = me + 1 - 2 * x
    y_mate = me + 2 - 4 * y
    z_next = me + group
    has_next = z_next < blocks
    has_prev = me >= group
    has_far = me >= 2 * group
    first_row = y == 0
    second_row = y == 1

    def local(index, src, dst):
        return pltpu.make_async_copy(src, dst, local_sems.at[index])

    def copy(kind, message, src, dst, device):
        return pltpu.make_async_remote_copy(
            src_ref=src,
            dst_ref=dst,
            send_sem=send_sems.at[kind],
            recv_sem=recv_sems.at[message],
            device_id=device,
            device_id_type=pl.DeviceIdType.MESH,
        )

    to_x = {"seq": x_mate}
    to_y = {"seq": y_mate}
    to_z = {"seq": z_next}
    to_core = {"head": 1 - side}

    def chunk(p):
        return pl.ds(pl.multiple_of(p * part, part), part)

    given = other
    sums = (branch, out_ref)
    halves = (side, 1 - side)
    pairs = (x, 1 - x)

    own_copy = [local(L_TOKEN + p, tokens_hbm.at[chunk(p)], own.at[chunk(p)]) for p in range(CHUNKS)]
    gain_copy = local(L_GAIN, gain_hbm, gain)
    freq_copy = local(L_FREQ, freq_hbm, freq)
    post_copy = local(L_POST, post_hbm, post)
    kv_copies = [[], []]
    q_copies = [[], []]
    out_copies = [[], []]
    for i in range(2):
        for f in range(2):
            at_rows = pl.ds(pl.multiple_of(halves[f] * width, width), width)
            for n, source in enumerate((wk_hbm, wv_hbm)):
                columns = pl.ds(pl.multiple_of(pairs[i] * HD, HD), HD)
                kv_copies[i].append(
                    local(
                        L_KV + i,
                        source.at[at_rows, columns],
                        wkv.at[i, pl.ds(f * width, width), pl.ds(n * HD, HD)],
                    )
                )
            columns = pl.ds(pl.multiple_of(pairs[i] * 2 * HD, 2 * HD), 2 * HD)
            q_copies[i].append(
                local(
                    L_Q + i,
                    wq_hbm.at[at_rows, columns],
                    wq.at[i, pl.ds(f * width, width), :],
                )
            )
            at_heads = pl.ds(pl.multiple_of(pairs[i] * 2 * HD, 2 * HD), 2 * HD)
            columns = pl.ds(pl.multiple_of(halves[1 - f] * width, width), width)
            out_copies[i].append(local(L_OUT, wo_hbm.at[at_heads, columns], wo.at[i, f]))

    order = [CHUNKS - 1 - i for i in range(CHUNKS)]
    for p in order:
        own_copy[p].start()
    freq_copy.start()
    gain_copy.start()
    for c in kv_copies[0]:
        c.start()

    barrier = pltpu.get_barrier_semaphore()

    def greet(device):
        pl.semaphore_signal(barrier, inc=1, device_id=device, device_id_type=pl.DeviceIdType.MESH)

    greet(to_core)
    greet(to_x)
    greet(to_y)
    pl.when(has_next)(lambda: greet(to_z))
    pl.when(has_prev)(lambda: greet({"seq": me - group}))
    pl.semaphore_wait(barrier, 3 + has_next.astype(jnp.int32) + has_prev.astype(jnp.int32))

    def token_copy(p):
        return copy(S_TOKEN, TOKEN + p, own.at[chunk(p)], other.at[chunk(p)], to_core)

    for p in order:
        own_copy[p].wait()
        token_copy(p).start()
    for c in kv_copies[1]:
        c.start()
    for i in (1, 0):
        for c in q_copies[i]:
            c.start()

    def piece(ref, p):
        return ref.at[:, chunk(p), :]

    def of(r):
        return x + r - 2 * x * r

    def send_x(p):
        return copy(S_X, X_KV + p, piece(kvm, p), piece(held.at[0, x], p), to_x)

    def take_x(p):
        return copy(S_X, X_KV + p, piece(kvm, p), piece(held.at[0, 1 - x], p), to_x)

    def place(r, p):
        return r * CHUNKS + CHUNKS - 1 - p

    def move(kind, message, src, dst, b, p, device):
        return copy(kind, message, piece(held.at[src, b], p), piece(held.at[dst, b], p), device)

    def z_near(r, p):
        return move(S_Z_NEAR, Z_NEAR + place(r, p), 0, 2, of(r), p, to_z)

    def z_far(b, p):
        return move(S_Z_FAR, Z_FAR + place(1 - b, p), 2, 4, b, p, to_z)

    def z_extra(p):
        return move(S_Z_FAR, Z_EXTRA + p, 1 + 2 * y, 3 + 2 * y, 0, p, to_z)

    def y_near(src, r, p):
        return move(S_Y_NEAR, Y_NEAR + place(r, p) // (CHUNKS // UNITS), src, 1, of(r), p, to_y)

    def y_far(src, b, p):
        kind = S_Y_FAR if b == 1 else S_Y_LATE
        return move(kind, Y_FAR + place(1 - b, p) // (CHUNKS // UNITS), src, 3, b, p, to_y)

    def y_extra(p):
        return move(S_Y_EXTRA, Y_EXTRA, 3 + 2 * y, 4, 0, p, to_y)

    def rows_of(h):
        return pl.ds(pl.multiple_of(h * unit, unit), unit)

    def take_unit(message, slot, b, h):
        block = held.at[slot, b, :, rows_of(h), :]
        copy(S_Y_NEAR, message, block, block, to_y).wait_recv()

    freq_copy.wait()
    at_row = lax.broadcasted_iota(jnp.int32, (rows, LANES), 0) + me * rows
    angles = at_row.astype(jnp.float32) * freq[...]
    cosine[...] = jnp.cos(angles)
    sine[...] = jnp.sin(angles)
    gain_copy.wait()

    lines = 16
    rounds = 4
    tiles = width // LANES

    def norm_chunk(p):
        def step(i, carry):
            start = p * part + i * lines * rounds
            spots = [
                pl.ds(pl.multiple_of(start + n * lines, lines), lines) for n in range(rounds)
            ]
            scales = []
            for at in spots:
                squares = None
                for ref in (own, other):
                    for j in range(tiles):
                        value = ref[at, j * LANES : (j + 1) * LANES].astype(jnp.float32)
                        squares = value * value if squares is None else squares + value * value
                scale = lax.rsqrt(
                    jnp.sum(squares, axis=-1, keepdims=True) / (2 * width) + norm_epsilon
                )
                scales.append(jnp.broadcast_to(scale, (lines, LANES)))
            for f, ref in enumerate((own, other)):
                for j in range(tiles):
                    weight = gain[pl.ds(halves[f] * tiles + j, 1), :]
                    to = f * width + j * LANES
                    for at, scale in zip(spots, scales):
                        value = ref[at, j * LANES : (j + 1) * LANES].astype(jnp.float32)
                        normed[at, to : to + LANES] = (value * scale * weight).astype(jnp.bfloat16)
            return carry

        lax.fori_loop(0, part // (lines * rounds), step, 0)

    def project_kv(p, i, dst):
        value = jnp.dot(normed[chunk(p), :], wkv[i], preferred_element_type=jnp.float32)
        key = rotated(value[:, :HD], cosine[chunk(p), :], sine[chunk(p), :])
        dst[0, chunk(p), :] = key
        dst[1, chunk(p), :] = value[:, HD:].astype(jnp.bfloat16)

    def take_near(r, p):
        def act():
            z_near(r, p).wait_recv()
            pl.when(second_row)(lambda: y_near(2, r, p).start())

        pl.when(has_prev)(act)

    far_order = [(1, 3), (1, 2), (1, 1), (1, 0), (0, 3), (0, 2)]
    late_order = [(0, 1), (0, 0), (1, 1), (1, 0), (0, 3), (0, 2)]

    def take_far(k):
        b, p = far_order[k]

        def act():
            z_far(b, p).wait_recv()
            pl.when(second_row)(lambda: y_far(4, b, p).start())

        pl.when(has_far)(act)

    def take_extra(p):
        def act():
            z_extra(p).wait_recv()
            y_extra(p).start()

        pl.when(has_far)(act)

    def pass_extra(row):
        def act():
            for p in (1, 0):
                z_extra(p).start()

        pl.when(has_next & has_prev & (y == row))(act)

    def pass_mate(p):
        take_x(p).wait_recv()
        pl.when(has_next)(lambda: z_near(1, p).start())
        pl.when(first_row)(lambda: y_near(0, 1, p).start())

    for i, p in enumerate(order):
        token_copy(p).wait_recv()
        norm_chunk(p)
        if i == 0:
            local(L_KV, wkv.at[0], wkv.at[0]).wait()
        project_kv(p, 0, held.at[0, x])
        pl.when(has_next)(lambda: z_near(0, p).start())
        pl.when(first_row)(lambda: y_near(0, 0, p).start())
        if i == 0:
            local(L_KV + 1, wkv.at[1], wkv.at[1]).wait()
        project_kv(p, 1, kvm)
        send_x(p).start()
        if i == 0:
            for i_ in (0, 1):
                for c in out_copies[i_]:
                    c.start()
            post_copy.start()
        if i == 2:
            take_near(0, order[0])

    def project_q(i, dst):
        def step(t, carry):
            at = pl.ds(pl.multiple_of(t * unit, unit), unit)
            value = jnp.dot(normed[at, :], wq[i], preferred_element_type=jnp.float32)
            for head in range(2):
                dst[pl.ds(pl.multiple_of(head * rows + t * unit, unit), unit), :] = rotated(
                    value[:, head * HD : (head + 1) * HD], cosine[at, :], sine[at, :]
                )
            return carry

        lax.fori_loop(0, UNITS, step, 0)

    def q_copy():
        return copy(S_Q, X_Q, asked, queries.at[1], to_x)

    total[...] = jnp.zeros_like(total)
    mass[...] = jnp.zeros_like(mass)
    pass_mate(order[0])
    local(L_Q + 1, wq.at[1], wq.at[1]).wait()
    take_near(0, order[1])
    project_q(1, asked)
    q_copy().start()
    pass_mate(order[1])
    take_near(0, order[2])
    local(L_Q + 0, wq.at[0], wq.at[0]).wait()
    project_q(0, queries.at[0])
    pass_mate(order[2])
    take_near(0, order[3])
    pass_mate(order[3])

    def attend(which, slot, b, h, distance=None):
        at = pl.ds(pl.multiple_of(h * unit, unit), unit)
        scores = lax.dot_general(
            queries[which],
            held[slot, b, 0, at, :],
            (((1,), (1,)), ((), ())),
            preferred_element_type=jnp.float32,
        )
        weights = jnp.exp2(outer * jnp.tanh(scores * inner))
        if distance is not None:
            down = lax.broadcasted_iota(jnp.int32, weights.shape, 0)
            down = jnp.where(down >= rows, down - rows, down)
            offset = (distance - h * unit) + down - lax.broadcasted_iota(jnp.int32, weights.shape, 1)
            weights = jnp.where((offset >= 0) & (offset < WINDOW), weights, 0.0)
        added = None
        for k in range(unit // LANES):
            lanes = weights[:, k * LANES : (k + 1) * LANES]
            added = lanes if added is None else added + lanes
        mass[which] += added
        total[which] += jnp.dot(
            weights.astype(jnp.bfloat16), held[slot, b, 1, at, :], preferred_element_type=jnp.float32
        )

    def both(act):
        def step(s, carry):
            act(s)
            return carry

        lax.fori_loop(0, 2, step, 0)

    def attend_own(which):
        mine = of(which)

        def step(i, carry):
            b = mine - i // UNITS
            attend(which, 0, b, i % UNITS, (mine - b) * rows)
            return carry

        lax.fori_loop(0, UNITS + UNITS * mine, step, 0)

    def z_unit(u):
        return 2, of(u // UNITS), UNITS - 1 - u % UNITS

    def y_unit(w):
        return 1, of(w // UNITS), UNITS - 1 - w % UNITS

    near_there = me >= 2
    far_there = me >= 6

    def take_y(w):
        take_unit(Y_NEAR + w, *y_unit(w))

    attend_own(0)

    def near_step(u, carry):
        p = CHUNKS - 1 - u
        take_near(1, p)
        pl.when(has_prev & has_next)(lambda: z_far(1, p).start())
        pl.when(has_prev & first_row & (u < 2))(lambda: y_far(2, 1, p).start())
        pl.when(has_prev)(lambda: attend(0, *z_unit(u)))

        def with_y():
            take_y(u - 1)
            attend(0, *y_unit(u - 1))

        pl.when((u >= 1) & near_there)(with_y)
        return carry

    lax.fori_loop(0, CHUNKS, near_step, 0)

    def pass_rest():
        for p in (3, 2):
            pl.when(has_next)(lambda: z_far(0, p).start())
        for b, p in late_order:
            pl.when(first_row)(lambda: y_far(2, b, p).start())

    pl.when(has_prev)(pass_rest)

    q_copy().wait_recv()
    attend_own(1)
    take_far(0)

    def again_z(u, carry):
        attend(1, *z_unit(u))
        return carry

    def again_y(w, carry):
        attend(1, *y_unit(w))
        return carry

    def repeat(count, step):
        def act():
            lax.fori_loop(0, count, step, 0)

        return act

    pl.when(has_prev)(repeat(4, again_z))
    take_far(1)
    pl.when(near_there)(repeat(3, again_y))

    def last_near():
        take_y(3)
        both(lambda s: attend(s, *y_unit(3)))

    pl.when(near_there)(last_near)
    pass_extra(0)

    third_b = (1, 1 - y, y, 0)
    third_h = (1, 0, 1 - y, y)

    def take_third(j):
        def act():
            message = Y_FAR + 2 * (1 - third_b[j]) + 1 - third_h[j]
            take_unit(message, 3, third_b[j], third_h[j])

        pl.when(far_there & ((j < 3) | second_row))(act)

    def third(j):
        pl.when(far_there)(lambda: both(lambda s: attend(s, 3, third_b[j], third_h[j])))

    def fourth(b, h):
        def act():
            def one(s):
                mine = of(s)
                pl.when(mine <= b)(lambda: attend(s, 4, b, h, WINDOW + (mine - b) * rows))

            both(one)

        pl.when(has_far)(act)

    take_far(2)
    fourth(1, 1)
    take_third(0)
    third(0)
    take_far(3)
    fourth(1, 0)
    pl.when(second_row)(lambda: take_third(1))
    pass_extra(1)
    take_far(4)
    pl.when(first_row)(lambda: take_third(1))
    third(1)
    take_far(5)
    fourth(0, 1)
    pl.when(second_row)(lambda: take_third(2))
    pl.when(second_row)(lambda: third(2))
    take_extra(1)
    pl.when(first_row)(lambda: take_third(2))
    pl.when(first_row)(lambda: third(2))
    take_extra(0)
    take_third(3)
    pl.when(far_there)(lambda: attend(1, 3, third_b[3], third_h[3]))

    def finish(which, head, at_rows):
        at = pl.ds(head * rows + at_rows.start, at_rows.size)
        weight = jnp.sum(mass[which, at, :], axis=-1, keepdims=True)
        return (total[which, at, :] * (1.0 / weight)).astype(jnp.bfloat16)

    def out_copy(p):
        return copy(S_OUT, X_OUT + p, leaving.at[chunk(p)], landed.at[chunk(p)], to_x)

    def send_out(p):
        for head in range(2):
            leaving[chunk(p), head * HD : (head + 1) * HD] = finish(1, head, chunk(p))
        out_copy(p).start()

    def project_own(h):
        at = slice(h * unit, (h + 1) * unit)
        for p in range(h * CHUNKS // UNITS, (h + 1) * CHUNKS // UNITS):
            for head in range(2):
                finished[chunk(p), head * HD : (head + 1) * HD] = finish(0, head, chunk(p))
        for f in range(2):
            sums[f][at, :] = jnp.dot(
                finished[at, :], wo[0, f], preferred_element_type=jnp.float32
            )

    def send_low():
        send_out(1)
        send_out(0)

    send_out(3)
    send_out(2)
    pl.when(x == 0)(send_low)
    pl.when(far_there)(lambda: attend(0, 3, third_b[3], third_h[3]))
    local(L_OUT, wo, wo).wait()
    post_copy.wait()
    project_own(1)

    def last_far():
        take_unit(Y_EXTRA, 4, 0, 0)
        attend(x, 4, 0, 0, WINDOW)

    pl.when(has_far)(last_far)
    pl.when(x == 1)(send_low)
    project_own(0)

    def given_copy(p):
        return copy(S_GIVEN, GIVEN + p, given.at[chunk(p)], arrived.at[chunk(p)], to_core)

    def squares_copy(p):
        return copy(S_SQUARES, SQUARES + p, sq_own.at[chunk(p)], sq_other.at[chunk(p)], to_core)

    def add_mate(p):
        out_copy(p).wait_recv()
        theirs = landed[chunk(p), :]
        given[chunk(p), :] = (
            branch[chunk(p), :]
            + jnp.dot(theirs, wo[1, 0], preferred_element_type=jnp.float32)
        ).astype(jnp.bfloat16)
        given_copy(p).start()
        out_ref[chunk(p), :] += jnp.dot(theirs, wo[1, 1], preferred_element_type=jnp.float32)

    def groups(p):
        return [pl.ds(p * part + n * lines, lines) for n in range(part // lines)]

    columns = [slice(j * LANES, (j + 1) * LANES) for j in range(tiles)]

    def add_core(p):
        given_copy(p).wait_recv()
        for rows_at in groups(p):
            shares = [out_ref[rows_at, at] + arrived[rows_at, at].astype(jnp.float32) for at in columns]
            squares = None
            for at, share in zip(columns, shares):
                out_ref[rows_at, at] = share
                squares = share * share if squares is None else squares + share * share
            sq_own[rows_at, :] = squares
        squares_copy(p).start()

    def last(p):
        squares_copy(p).wait_recv()
        for rows_at in groups(p):
            squares = jnp.sum(sq_own[rows_at, :] + sq_other[rows_at, :], axis=-1, keepdims=True)
            scale = jnp.broadcast_to(
                lax.rsqrt(squares / (2 * width) + norm_epsilon), (lines, LANES)
            )
            values = [
                post[j : j + 1, :] * out_ref[rows_at, at] * scale for j, at in enumerate(columns)
            ]
            for at, value in zip(columns, values):
                out_ref[rows_at, at] = value

    def tail(i, carry):
        p = CHUNKS - 1 - i
        pl.when(i < CHUNKS)(lambda: add_mate(p))
        pl.when((i >= 1) & (i < CHUNKS + 1))(lambda: add_core(p + 1))
        pl.when(i >= 2)(lambda: last(p + 2))
        return carry

    lax.fori_loop(0, CHUNKS + 2, tail, 0)

    def sent(kind, ref):
        copy(kind, TOKEN, ref, ref, to_x).wait_send()

    block = held.at[0, 0]
    sent(S_TOKEN, own)
    sent(S_X, kvm)
    sent(S_Q, asked)
    sent(S_OUT, leaving)
    sent(S_GIVEN, given)
    sent(S_SQUARES, sq_own)
    pl.when(has_next)(lambda: sent(S_Z_NEAR, held.at[0]))
    pl.when(has_next & has_prev)(lambda: sent(S_Z_FAR, held.at[0]))
    pl.when(first_row | has_prev)(lambda: sent(S_Y_NEAR, held.at[0]))
    pl.when((first_row & has_prev) | has_far)(lambda: sent(S_Y_FAR, block))
    pl.when(first_row & has_prev)(lambda: sent(S_Y_LATE, block))
    pl.when(second_row & has_far)(lambda: sent(S_Y_LATE, block.at[:, rows_of(0), :]))
    pl.when(has_far)(lambda: sent(S_Y_EXTRA, block.at[:, rows_of(0), :]))


def local_layer(blocks, tokens, pre_gain, query_weight, key_weight, value_weight, out_weight, post_gain):
    rows, width = tokens.shape
    frequency = np.exp(-np.log(rope_base) * (2.0 * np.arange(HD // 2) / HD)).astype(np.float32)
    anywhere = pl.BlockSpec(memory_space=pltpu.HBM)
    bf16, f32 = jnp.bfloat16, jnp.float32
    vmem = pltpu.VMEM
    half = 2 * HD
    normed_branch = pl.pallas_call(
        functools.partial(layer_kernel, blocks),
        out_shape=vmem((rows, width), f32),
        in_specs=[anywhere] * 8,
        out_specs=pl.BlockSpec(memory_space=pltpu.VMEM),
        scratch_shapes=[
            vmem((rows, width), bf16),
            vmem((rows, width), bf16),
            vmem((2 * width // LANES, LANES), f32),
            vmem((1, LANES), f32),
            vmem((width // LANES, LANES), f32),
            vmem((rows, 2 * width), bf16),
            vmem((2, 2 * width, half), bf16),
            vmem((2, 2 * width, half), bf16),
            vmem((2, 2, half, width), bf16),
            vmem((rows, LANES), f32),
            vmem((rows, LANES), f32),
            vmem((6, 2, 2, rows, HD), bf16),
            vmem((2, rows, HD), bf16),
            vmem((2, 2 * rows, HD), bf16),
            vmem((2 * rows, HD), bf16),
            vmem((2, 2 * rows, HD), f32),
            vmem((2, 2 * rows, LANES), f32),
            vmem((rows, half), bf16),
            vmem((rows, half), bf16),
            vmem((rows, half), bf16),
            vmem((rows, width), f32),
            vmem((rows, width), bf16),
            vmem((rows, LANES), f32),
            vmem((rows, LANES), f32),
            pltpu.SemaphoreType.DMA((SENDS,)),
            pltpu.SemaphoreType.DMA((MESSAGES,)),
            pltpu.SemaphoreType.DMA((LOCALS,)),
        ],
        compiler_params=pltpu.CompilerParams(
            collective_id=0, has_side_effects=True, vmem_limit_bytes=56 * 1024 * 1024
        ),
    )(
        tokens,
        pre_gain.reshape(-1, LANES),
        jnp.asarray(frequency)[None, :],
        query_weight,
        key_weight,
        value_weight,
        out_weight,
        post_gain.reshape(-1, LANES),
    )
    return (tokens.astype(f32) + normed_branch).astype(bf16)


def solution(mesh):
    placed = (
        P("seq", "head"),
        P(),
        P(None, "head"),
        P(None, "head"),
        P(None, "head"),
        P("head", None),
        P("head"),
    )
    return jax.shard_map(
        functools.partial(local_layer, mesh.shape["seq"]),
        mesh=mesh,
        in_specs=placed,
        out_specs=P("seq", "head"),
        check_vma=False,
    )
```

```python
import functools
import math

import jax
import jax.numpy as jnp
import numpy as np
from jax import lax
from jax.experimental import pallas as pl
from jax.experimental.pallas import tpu as pltpu
from jax.sharding import PartitionSpec as P

HD = 256
LANES = 128
WINDOW = 4096

softcap_limit = 50.0
rope_base = 10000.0
norm_epsilon = 1e-06

CHUNKS = 4

SLABS = ((12, 4), (8, 4), (4, 4), (2, 2), (0, 2))
OUTS = len(SLABS)

STEPS = ((3, 14, 2), (3, 12, 2), (2, 8, 4), (1, 4, 4), (0, 0, 4))
UNITS = 2

TOKEN = 0
X_KV = TOKEN + len(STEPS)
X_Q = X_KV + CHUNKS
X_OUT = X_Q + 1
Z_NEAR = X_OUT + OUTS
Z_FAR = Z_NEAR + 2 * CHUNKS
Z_EXTRA = Z_FAR + CHUNKS + CHUNKS // 2
Y_NEAR = Z_EXTRA + CHUNKS // 2
Y_FAR = Y_NEAR + 2 * UNITS
Y_EXTRA = Y_FAR + 2 * UNITS
GIVEN = Y_EXTRA + 1
SQUARES = GIVEN + OUTS
MESSAGES = SQUARES + OUTS

(
    S_TOKEN, S_X, S_Q, S_OUT, S_Z_NEAR, S_Z_FAR, S_Y_NEAR, S_Y_FAR, S_Y_LATE, S_Y_EXTRA, S_GIVEN,
    S_SQUARES, SENDS,
) = range(13)

L_TOKEN = 0
L_GAIN = L_TOKEN + len(STEPS)
L_FREQ = L_GAIN + 1
L_POST = L_FREQ + 1
L_KV = L_POST + 1
L_Q = L_KV + 2
L_OUT = L_Q + 2
LOCALS = L_OUT + 1

inner = 1.0 / (math.sqrt(HD) * softcap_limit)
outer = softcap_limit / math.log(2.0)


def rotated(head, cosine, sine):
    midpoint = HD // 2
    leading, trailing = head[:, :midpoint], head[:, midpoint:]
    return jnp.concatenate(
        [leading * cosine - trailing * sine, trailing * cosine + leading * sine], axis=-1
    ).astype(jnp.bfloat16)


def layer_kernel(
    blocks, tokens_hbm, gain_hbm, freq_hbm, wq_hbm, wk_hbm, wv_hbm, wo_hbm, post_hbm, out_ref,
    own, other, gain, freq, post, normed, wkv, wq, wo, cosine, sine, held, kvm, queries, asked,
    total, mass, leaving, landed, finished, branch, kept, arrived, sq_own, sq_other,
    send_sems, recv_sems, local_sems,
):
    rows, width = own.shape
    part = rows // CHUNKS
    unit = rows // UNITS
    group = 2 * 2
    me = lax.axis_index("seq")
    side = lax.axis_index("head")
    x = me % 2
    y = (me // 2) % 2
    x_mate = me + 1 - 2 * x
    y_mate = me + 2 - 4 * y
    z_next = me + group
    has_next = z_next < blocks
    has_prev = me >= group
    has_far = me >= 2 * group
    first_row = y == 0
    second_row = y == 1

    def local(index, src, dst):
        return pltpu.make_async_copy(src, dst, local_sems.at[index])

    def copy(kind, message, src, dst, device):
        return pltpu.make_async_remote_copy(
            src_ref=src,
            dst_ref=dst,
            send_sem=send_sems.at[kind],
            recv_sem=recv_sems.at[message],
            device_id=device,
            device_id_type=pl.DeviceIdType.MESH,
        )

    to_x = {"seq": x_mate}
    to_y = {"seq": y_mate}
    to_z = {"seq": z_next}
    to_core = {"head": 1 - side}

    def chunk(p):
        return pl.ds(pl.multiple_of(p * part, part), part)

    given = other
    sums = (branch, kept)
    halves = (side, 1 - side)
    pairs = (x, 1 - x)

    steps = [
        (p, pl.ds(first * rows // 16, size * rows // 16)) for p, first, size in STEPS
    ]
    own_copy = [
        local(L_TOKEN + i, tokens_hbm.at[at], own.at[at]) for i, (_, at) in enumerate(steps)
    ]
    gain_copy = local(L_GAIN, gain_hbm, gain)
    freq_copy = local(L_FREQ, freq_hbm, freq)
    post_copy = local(L_POST, post_hbm, post)
    kv_copies = [[], []]
    q_copies = [[], []]
    out_copies = [[], []]
    for i in range(2):
        for f in range(2):
            at_rows = pl.ds(pl.multiple_of(halves[f] * width, width), width)
            for n, source in enumerate((wk_hbm, wv_hbm)):
                columns = pl.ds(pl.multiple_of(pairs[i] * HD, HD), HD)
                kv_copies[i].append(
                    local(
                        L_KV + i,
                        source.at[at_rows, columns],
                        wkv.at[i, pl.ds(f * width, width), pl.ds(n * HD, HD)],
                    )
                )
            columns = pl.ds(pl.multiple_of(pairs[i] * 2 * HD, 2 * HD), 2 * HD)
            q_copies[i].append(
                local(
                    L_Q + i,
                    wq_hbm.at[at_rows, columns],
                    wq.at[i, pl.ds(f * width, width), :],
                )
            )
            at_heads = pl.ds(pl.multiple_of(pairs[i] * 2 * HD, 2 * HD), 2 * HD)
            columns = pl.ds(pl.multiple_of(halves[1 - f] * width, width), width)
            out_copies[i].append(local(L_OUT, wo_hbm.at[at_heads, columns], wo.at[i, f]))

    order = [CHUNKS - 1 - i for i in range(CHUNKS)]
    for c in own_copy[:2]:
        c.start()
    freq_copy.start()
    gain_copy.start()
    for c in kv_copies[0]:
        c.start()
    for c in own_copy[2:]:
        c.start()

    barrier = pltpu.get_barrier_semaphore()

    def greet(device):
        pl.semaphore_signal(barrier, inc=1, device_id=device, device_id_type=pl.DeviceIdType.MESH)

    greet(to_core)
    greet(to_x)
    greet(to_y)
    pl.when(has_next)(lambda: greet(to_z))
    pl.when(has_prev)(lambda: greet({"seq": me - group}))
    pl.semaphore_wait(barrier, 3 + has_next.astype(jnp.int32) + has_prev.astype(jnp.int32))

    def token_copy(i):
        at = steps[i][1]
        return copy(S_TOKEN, TOKEN + i, own.at[at], other.at[at], to_core)

    for i in range(2):
        own_copy[i].wait()
        token_copy(i).start()
    for c in kv_copies[1]:
        c.start()

    def piece(ref, p):
        return ref.at[:, chunk(p), :]

    def of(r):
        return x + r - 2 * x * r

    def send_x(p):
        return copy(S_X, X_KV + p, piece(kvm, p), piece(held.at[0, x], p), to_x)

    def take_x(p):
        return copy(S_X, X_KV + p, piece(kvm, p), piece(held.at[0, 1 - x], p), to_x)

    def place(r, p):
        return r * CHUNKS + CHUNKS - 1 - p

    def move(kind, message, src, dst, b, p, device):
        return copy(kind, message, piece(held.at[src, b], p), piece(held.at[dst, b], p), device)

    def z_near(r, p):
        return move(S_Z_NEAR, Z_NEAR + place(r, p), 0, 2, of(r), p, to_z)

    def z_far(b, p):
        return move(S_Z_FAR, Z_FAR + place(1 - b, p), 2, 4, b, p, to_z)

    def z_extra(p):
        return move(S_Z_FAR, Z_EXTRA + p, 1 + 2 * y, 3 + 2 * y, 0, p, to_z)

    def y_near(src, r, p):
        return move(S_Y_NEAR, Y_NEAR + place(r, p) // (CHUNKS // UNITS), src, 1, of(r), p, to_y)

    def y_far(src, b, p):
        kind = S_Y_FAR if b == 1 else S_Y_LATE
        return move(kind, Y_FAR + place(1 - b, p) // (CHUNKS // UNITS), src, 3, b, p, to_y)

    def y_extra(p):
        return move(S_Y_EXTRA, Y_EXTRA, 3 + 2 * y, 4, 0, p, to_y)

    def rows_of(h):
        return pl.ds(pl.multiple_of(h * unit, unit), unit)

    def take_unit(message, slot, b, h):
        block = held.at[slot, b, :, rows_of(h), :]
        copy(S_Y_NEAR, message, block, block, to_y).wait_recv()

    freq_copy.wait()

    def turn(at):
        at_row = lax.broadcasted_iota(jnp.int32, (at.size, LANES), 0) + (me * rows + at.start)
        angles = at_row.astype(jnp.float32) * freq[...]
        cosine[at, :] = jnp.cos(angles)
        sine[at, :] = jnp.sin(angles)

    turn(pl.ds(order[0] * part, part))
    gain_copy.wait()
    for i in range(2, len(steps)):
        own_copy[i].wait()
        token_copy(i).start()
    for i in (1, 0):
        for c in q_copies[i]:
            c.start()

    lines = 16
    rounds = 4
    tiles = width // LANES

    def norm_chunk(rows_at):
        def step(i, carry):
            start = rows_at.start + i * lines * rounds
            spots = [
                pl.ds(pl.multiple_of(start + n * lines, lines), lines) for n in range(rounds)
            ]
            scales = []
            for at in spots:
                squares = None
                for ref in (own, other):
                    for j in range(tiles):
                        value = ref[at, j * LANES : (j + 1) * LANES].astype(jnp.float32)
                        squares = value * value if squares is None else squares + value * value
                scale = lax.rsqrt(
                    jnp.sum(squares, axis=-1, keepdims=True) / (2 * width) + norm_epsilon
                )
                scales.append(jnp.broadcast_to(scale, (lines, LANES)))
            for f, ref in enumerate((own, other)):
                for j in range(tiles):
                    weight = gain[pl.ds(halves[f] * tiles + j, 1), :]
                    to = f * width + j * LANES
                    for at, scale in zip(spots, scales):
                        value = ref[at, j * LANES : (j + 1) * LANES].astype(jnp.float32)
                        normed[at, to : to + LANES] = (value * scale * weight).astype(jnp.bfloat16)
            return carry

        lax.fori_loop(0, rows_at.size // (lines * rounds), step, 0)

    def project_kv(at, i, dst):
        value = jnp.dot(normed[at, :], wkv[i], preferred_element_type=jnp.float32)
        key = rotated(value[:, :HD], cosine[at, :], sine[at, :])
        dst[0, at, :] = key
        dst[1, at, :] = value[:, HD:].astype(jnp.bfloat16)

    def take_near(r, p):
        def act():
            z_near(r, p).wait_recv()
            pl.when(second_row)(lambda: y_near(2, r, p).start())

        pl.when(has_prev)(act)

    far_order = [(1, 3), (1, 2), (1, 1), (1, 0), (0, 3), (0, 2)]
    late_order = [(0, 1), (0, 0), (1, 1), (1, 0), (0, 3), (0, 2)]

    def take_far(k):
        b, p = far_order[k]

        def act():
            z_far(b, p).wait_recv()
            pl.when(second_row)(lambda: y_far(4, b, p).start())

        pl.when(has_far)(act)

    def take_extra(p):
        def act():
            z_extra(p).wait_recv()
            y_extra(p).start()

        pl.when(has_far)(act)

    def pass_extra(row):
        def act():
            for p in (1, 0):
                z_extra(p).start()

        pl.when(has_next & has_prev & (y == row))(act)

    def pass_mate(p):
        take_x(p).wait_recv()
        pl.when(has_next)(lambda: z_near(1, p).start())
        pl.when(first_row)(lambda: y_near(0, 1, p).start())

    def rows_copy(kind, message, src, dst, at, device):
        copy(kind, message, src.at[:, at, :], dst.at[:, at, :], device).start()

    for i, (p, at) in enumerate(steps):
        token_copy(i).wait_recv()
        norm_chunk(at)
        if i > 1:
            turn(at)
        if i == 0:
            local(L_KV, wkv.at[0], wkv.at[0]).wait()
        project_kv(at, 0, held.at[0, x])

        def near_rows(slot, kind, message, device):
            rows_copy(kind, message, held.at[0, x], held.at[slot, x], at, device)

        pl.when(has_next)(lambda: near_rows(2, S_Z_NEAR, Z_NEAR + place(0, p), to_z))
        pl.when(first_row)(
            lambda: near_rows(1, S_Y_NEAR, Y_NEAR + place(0, p) // (CHUNKS // UNITS), to_y)
        )
        if i == 0:
            continue
        if i == 4:
            take_near(0, order[1])
        if i == 1:
            local(L_KV + 1, wkv.at[1], wkv.at[1]).wait()
            for c in out_copies[0] + out_copies[1]:
                c.start()
            post_copy.start()
        project_kv(pl.ds(p * part, part), 1, kvm)
        send_x(p).start()
        if i == 2:
            take_near(0, order[0])

    def project_q(i, dst):
        def step(t, carry):
            at = pl.ds(pl.multiple_of(t * unit, unit), unit)
            value = jnp.dot(normed[at, :], wq[i], preferred_element_type=jnp.float32)
            for head in range(2):
                dst[pl.ds(pl.multiple_of(head * rows + t * unit, unit), unit), :] = rotated(
                    value[:, head * HD : (head + 1) * HD], cosine[at, :], sine[at, :]
                )
            return carry

        lax.fori_loop(0, UNITS, step, 0)

    def q_copy():
        return copy(S_Q, X_Q, asked, queries.at[1], to_x)

    total[...] = jnp.zeros_like(total)
    mass[...] = jnp.zeros_like(mass)
    pass_mate(order[0])
    local(L_Q + 1, wq.at[1], wq.at[1]).wait()
    project_q(1, asked)
    q_copy().start()
    pass_mate(order[1])
    take_near(0, order[2])
    local(L_Q + 0, wq.at[0], wq.at[0]).wait()
    project_q(0, queries.at[0])
    pass_mate(order[2])
    take_near(0, order[3])
    pass_mate(order[3])

    def attend(which, slot, b, h, distance=None):
        at = pl.ds(pl.multiple_of(h * unit, unit), unit)
        scores = lax.dot_general(
            queries[which],
            held[slot, b, 0, at, :],
            (((1,), (1,)), ((), ())),
            preferred_element_type=jnp.float32,
        )
        weights = jnp.exp2(outer * jnp.tanh(scores * inner))
        if distance is not None:
            down = lax.broadcasted_iota(jnp.int32, weights.shape, 0)
            down = jnp.where(down >= rows, down - rows, down)
            offset = (distance - h * unit) + down - lax.broadcasted_iota(jnp.int32, weights.shape, 1)
            weights = jnp.where((offset >= 0) & (offset < WINDOW), weights, 0.0)
        added = None
        for k in range(unit // LANES):
            lanes = weights[:, k * LANES : (k + 1) * LANES]
            added = lanes if added is None else added + lanes
        mass[which] += added
        total[which] += jnp.dot(
            weights.astype(jnp.bfloat16), held[slot, b, 1, at, :], preferred_element_type=jnp.float32
        )

    def both(act):
        def step(s, carry):
            act(s)
            return carry

        lax.fori_loop(0, 2, step, 0)

    def attend_own(which):
        mine = of(which)

        def step(i, carry):
            b = mine - i // UNITS
            if which == 1:
                pl.when(i == 1)(lambda: take_far(0))
            attend(which, 0, b, i % UNITS, (mine - b) * rows)
            return carry

        lax.fori_loop(0, UNITS + UNITS * mine, step, 0)

    def z_unit(u):
        return 2, of(u // UNITS), UNITS - 1 - u % UNITS

    def y_unit(w):
        return 1, of(w // UNITS), UNITS - 1 - w % UNITS

    near_there = me >= 2
    far_there = me >= 6

    def take_y(w):
        take_unit(Y_NEAR + w, *y_unit(w))

    def near_pass(u):
        p = CHUNKS - 1 - u
        take_near(1, p)
        pl.when(has_prev & has_next)(lambda: z_far(1, p).start())
        pl.when(has_prev & first_row & (u < 2))(lambda: y_far(2, 1, p).start())

    near_pass(0)
    attend_own(0)

    def near_step(u, carry):
        pl.when(u >= 1)(lambda: near_pass(u))
        pl.when(has_prev)(lambda: attend(0, *z_unit(u)))

        def with_y():
            take_y(u - 1)
            attend(0, *y_unit(u - 1))

        pl.when((u >= 1) & near_there)(with_y)
        return carry

    lax.fori_loop(0, CHUNKS, near_step, 0)

    def pass_rest():
        for p in (3, 2):
            pl.when(has_next)(lambda: z_far(0, p).start())
        for b, p in late_order:
            pl.when(first_row)(lambda: y_far(2, b, p).start())

    pl.when(has_prev)(pass_rest)

    q_copy().wait_recv()
    attend_own(1)

    def again_z(u, carry):
        pl.when(u == 1)(lambda: take_far(1))
        attend(1, *z_unit(u))
        return carry

    def again_y(w, carry):
        pl.when(w == 2)(lambda: take_far(2))
        attend(1, *y_unit(w))
        return carry

    def repeat(count, step):
        def act():
            lax.fori_loop(0, count, step, 0)

        return act

    pl.when(has_prev)(repeat(4, again_z))
    pl.when(near_there)(repeat(3, again_y))

    def last_near():
        take_y(3)
        both(lambda s: attend(s, *y_unit(3)))

    pl.when(near_there)(last_near)
    pass_extra(0)

    third_b = (1, 1 - y, y, 0)
    third_h = (1, 0, 1 - y, y)

    def take_third(j):
        def act():
            message = Y_FAR + 2 * (1 - third_b[j]) + 1 - third_h[j]
            take_unit(message, 3, third_b[j], third_h[j])

        pl.when(far_there & ((j < 3) | second_row))(act)

    def third(j):
        pl.when(far_there)(lambda: both(lambda s: attend(s, 3, third_b[j], third_h[j])))

    def fourth(b, h):
        def act():
            def one(s):
                mine = of(s)
                pl.when(mine <= b)(lambda: attend(s, 4, b, h, WINDOW + (mine - b) * rows))

            both(one)

        pl.when(has_far)(act)

    take_far(3)
    fourth(1, 1)
    take_third(0)
    third(0)
    take_far(4)
    fourth(1, 0)
    pl.when(second_row)(lambda: take_third(1))
    pass_extra(1)
    pl.when(first_row)(lambda: take_third(1))
    third(1)
    take_far(5)
    fourth(0, 1)
    pl.when(second_row)(lambda: take_third(2))
    pl.when(second_row)(lambda: third(2))
    take_extra(1)
    pl.when(first_row)(lambda: take_third(2))

    def late(which):
        attend(which, 3, third_b[2], third_h[2])

    pl.when(far_there & first_row)(lambda: late(1))
    take_extra(0)
    take_third(3)
    pl.when(far_there)(lambda: attend(1, 3, third_b[3], third_h[3]))

    def slab(p):
        first, size = SLABS[p]
        return pl.ds(first * rows // 16, size * rows // 16)

    def finish(which, head, at_rows):
        at = pl.ds(head * rows + at_rows.start, at_rows.size)
        weight = jnp.sum(mass[which, at, :], axis=-1, keepdims=True)
        return (total[which, at, :] * (1.0 / weight)).astype(jnp.bfloat16)

    def out_copy(p):
        return copy(S_OUT, X_OUT + p, leaving.at[slab(p)], landed.at[slab(p)], to_x)

    def send_out(p):
        for head in range(2):
            leaving[slab(p), head * HD : (head + 1) * HD] = finish(1, head, slab(p))
        out_copy(p).start()

    def project_own(h):
        at = slice(h * unit, (h + 1) * unit)
        for p in (range(2) if h else range(2, OUTS)):
            for head in range(2):
                finished[slab(p), head * HD : (head + 1) * HD] = finish(0, head, slab(p))
        for f in range(2):
            sums[f][at, :] = jnp.dot(
                finished[at, :], wo[0, f], preferred_element_type=jnp.float32
            )

    def send_low():
        for p in range(2, OUTS):
            send_out(p)

    def send_high():
        for p in range(2):
            send_out(p)

    send_high()
    pl.when(x == 0)(send_low)
    pl.when(far_there & first_row)(lambda: late(0))
    pl.when(far_there)(lambda: attend(0, 3, third_b[3], third_h[3]))
    local(L_OUT, wo, wo).wait()
    post_copy.wait()
    project_own(1)

    def last_far():
        take_unit(Y_EXTRA, 4, 0, 0)
        attend(x, 4, 0, 0, WINDOW)

    pl.when(has_far)(last_far)
    pl.when(x == 1)(send_low)
    project_own(0)

    def given_copy(p):
        return copy(S_GIVEN, GIVEN + p, given.at[slab(p)], arrived.at[slab(p)], to_core)

    def squares_copy(p):
        return copy(S_SQUARES, SQUARES + p, sq_own.at[slab(p)], sq_other.at[slab(p)], to_core)

    def give(p):
        out_copy(p).wait_recv()
        given[slab(p), :] = (
            branch[slab(p), :]
            + jnp.dot(landed[slab(p), :], wo[1, 0], preferred_element_type=jnp.float32)
        ).astype(jnp.bfloat16)
        given_copy(p).start()

    def keep(p):
        kept[slab(p), :] += jnp.dot(
            landed[slab(p), :], wo[1, 1], preferred_element_type=jnp.float32
        )

    def groups(p):
        return [pl.ds(slab(p).start + n * lines, lines) for n in range(slab(p).size // lines)]

    columns = [slice(j * LANES, (j + 1) * LANES) for j in range(tiles)]

    def add_core(p):
        given_copy(p).wait_recv()
        for rows_at in groups(p):
            shares = [kept[rows_at, at] + arrived[rows_at, at].astype(jnp.float32) for at in columns]
            squares = None
            for at, share in zip(columns, shares):
                kept[rows_at, at] = share
                squares = share * share if squares is None else squares + share * share
            sq_own[rows_at, :] = squares
        squares_copy(p).start()

    def last(p):
        squares_copy(p).wait_recv()
        for rows_at in groups(p):
            squares = jnp.sum(sq_own[rows_at, :] + sq_other[rows_at, :], axis=-1, keepdims=True)
            scale = jnp.broadcast_to(
                lax.rsqrt(squares / (2 * width) + norm_epsilon), (lines, LANES)
            )
            values = [
                own[rows_at, at].astype(jnp.float32) + post[j : j + 1, :] * kept[rows_at, at] * scale
                for j, at in enumerate(columns)
            ]
            for at, value in zip(columns, values):
                out_ref[rows_at, at] = value.astype(jnp.bfloat16)

    for p in range(OUTS - 2):
        give(p)
        keep(p)
        if p >= 1:
            add_core(p - 1)
        if p >= 2:
            last(p - 2)
    give(OUTS - 2)
    add_core(OUTS - 3)
    last(OUTS - 4)
    give(OUTS - 1)
    keep(OUTS - 2)
    keep(OUTS - 1)
    last(OUTS - 3)
    add_core(OUTS - 2)
    add_core(OUTS - 1)
    last(OUTS - 2)
    last(OUTS - 1)

    def sent(kind, ref):
        copy(kind, TOKEN, ref, ref, to_x).wait_send()

    block = held.at[0, 0]
    sent(S_TOKEN, own)
    sent(S_X, kvm)
    sent(S_Q, asked)
    sent(S_OUT, leaving)
    sent(S_GIVEN, given)
    sent(S_SQUARES, sq_own)
    pl.when(has_next)(lambda: sent(S_Z_NEAR, held.at[0]))
    pl.when(has_next & has_prev)(lambda: sent(S_Z_FAR, held.at[0]))
    pl.when(first_row | has_prev)(lambda: sent(S_Y_NEAR, held.at[0]))
    pl.when((first_row & has_prev) | has_far)(lambda: sent(S_Y_FAR, block))
    pl.when(first_row & has_prev)(lambda: sent(S_Y_LATE, block))
    pl.when(second_row & has_far)(lambda: sent(S_Y_LATE, block.at[:, rows_of(0), :]))
    pl.when(has_far)(lambda: sent(S_Y_EXTRA, block.at[:, rows_of(0), :]))


def local_layer(blocks, tokens, pre_gain, query_weight, key_weight, value_weight, out_weight, post_gain):
    rows, width = tokens.shape
    frequency = np.exp(-np.log(rope_base) * (2.0 * np.arange(HD // 2) / HD)).astype(np.float32)
    anywhere = pl.BlockSpec(memory_space=pltpu.HBM)
    bf16, f32 = jnp.bfloat16, jnp.float32
    vmem = pltpu.VMEM
    half = 2 * HD
    normed_branch = pl.pallas_call(
        functools.partial(layer_kernel, blocks),
        out_shape=vmem((rows, width), bf16),
        in_specs=[anywhere] * 8,
        out_specs=pl.BlockSpec(memory_space=pltpu.VMEM),
        scratch_shapes=[
            vmem((rows, width), bf16),
            vmem((rows, width), bf16),
            vmem((2 * width // LANES, LANES), f32),
            vmem((1, LANES), f32),
            vmem((width // LANES, LANES), f32),
            vmem((rows, 2 * width), bf16),
            vmem((2, 2 * width, half), bf16),
            vmem((2, 2 * width, half), bf16),
            vmem((2, 2, half, width), bf16),
            vmem((rows, LANES), f32),
            vmem((rows, LANES), f32),
            vmem((6, 2, 2, rows, HD), bf16),
            vmem((2, rows, HD), bf16),
            vmem((2, 2 * rows, HD), bf16),
            vmem((2 * rows, HD), bf16),
            vmem((2, 2 * rows, HD), f32),
            vmem((2, 2 * rows, LANES), f32),
            vmem((rows, half), bf16),
            vmem((rows, half), bf16),
            vmem((rows, half), bf16),
            vmem((rows, width), f32),
            vmem((rows, width), f32),
            vmem((rows, width), bf16),
            vmem((rows, LANES), f32),
            vmem((rows, LANES), f32),
            pltpu.SemaphoreType.DMA((SENDS,)),
            pltpu.SemaphoreType.DMA((MESSAGES,)),
            pltpu.SemaphoreType.DMA((LOCALS,)),
        ],
        compiler_params=pltpu.CompilerParams(
            collective_id=0, has_side_effects=True, vmem_limit_bytes=58 * 1024 * 1024
        ),
    )(
        tokens,
        pre_gain.reshape(-1, LANES),
        jnp.asarray(frequency)[None, :],
        query_weight,
        key_weight,
        value_weight,
        out_weight,
        post_gain.reshape(-1, LANES),
    )
    return normed_branch


def solution(mesh):
    placed = (
        P("seq", "head"),
        P(),
        P(None, "head"),
        P(None, "head"),
        P(None, "head"),
        P("head", None),
        P("head"),
    )
    return jax.shard_map(
        functools.partial(local_layer, mesh.shape["seq"]),
        mesh=mesh,
        in_specs=placed,
        out_specs=P("seq", "head"),
        check_vma=False,
    )
```

```python
import functools
import math

import jax
import jax.numpy as jnp
import numpy as np
from jax import lax
from jax.experimental import pallas as pl
from jax.experimental.pallas import tpu as pltpu
from jax.sharding import PartitionSpec as P

HD = 256
LANES = 128
WINDOW = 4096

softcap_limit = 50.0
rope_base = 10000.0
norm_epsilon = 1e-06

CHUNKS = 4

SLABS = ((12, 4), (8, 4), (4, 4), (2, 2), (0, 2))
OUTS = len(SLABS)

STEPS = ((3, 14, 2), (3, 12, 2), (2, 8, 4), (1, 4, 4), (0, 0, 4))
UNITS = 2

TOKEN = 0
X_KV = TOKEN + len(STEPS)
X_Q = X_KV + CHUNKS
X_OUT = X_Q + 1
Z_NEAR = X_OUT + OUTS
Z_FAR = Z_NEAR + 2 * CHUNKS
Z_EXTRA = Z_FAR + CHUNKS + CHUNKS // 2
Y_NEAR = Z_EXTRA + CHUNKS // 2
Y_FAR = Y_NEAR + 2 * UNITS
Y_EXTRA = Y_FAR + 2 * UNITS
GIVEN = Y_EXTRA + 1
SQUARES = GIVEN + OUTS
MESSAGES = SQUARES + OUTS

(
    S_TOKEN, S_X, S_Q, S_OUT, S_Z_NEAR, S_Z_FAR, S_Y_NEAR, S_Y_FAR, S_Y_LATE, S_Y_EXTRA, S_GIVEN,
    S_SQUARES, SENDS,
) = range(13)

L_TOKEN = 0
L_GAIN = L_TOKEN + len(STEPS)
L_FREQ = L_GAIN + 1
L_POST = L_FREQ + 1
L_KV = L_POST + 1
L_Q = L_KV + 2
L_OUT = L_Q + 2
LOCALS = L_OUT + 1

inner = 1.0 / (math.sqrt(HD) * softcap_limit)
outer = softcap_limit / math.log(2.0)


def rotated(head, cosine, sine):
    midpoint = HD // 2
    leading, trailing = head[:, :midpoint], head[:, midpoint:]
    return jnp.concatenate(
        [leading * cosine - trailing * sine, trailing * cosine + leading * sine], axis=-1
    ).astype(jnp.bfloat16)


def layer_kernel(
    blocks, tokens_hbm, gain_hbm, freq_hbm, wq_hbm, wk_hbm, wv_hbm, wo_hbm, post_hbm, out_ref,
    own, other, gain, freq, post, normed, wkv, wq, wo, cosine, sine, held, kvm, queries, asked,
    total, mass, leaving, landed, finished, branch, kept, arrived, sq_own, sq_other,
    send_sems, recv_sems, local_sems,
):
    rows, width = own.shape
    part = rows // CHUNKS
    unit = rows // UNITS
    group = 2 * 2
    me = lax.axis_index("seq")
    side = lax.axis_index("head")
    x = me % 2
    y = (me // 2) % 2
    x_mate = me + 1 - 2 * x
    y_mate = me + 2 - 4 * y
    z_next = me + group
    has_next = z_next < blocks
    has_prev = me >= group
    has_far = me >= 2 * group
    first_row = y == 0
    second_row = y == 1

    def local(index, src, dst):
        return pltpu.make_async_copy(src, dst, local_sems.at[index])

    def copy(kind, message, src, dst, device):
        return pltpu.make_async_remote_copy(
            src_ref=src,
            dst_ref=dst,
            send_sem=send_sems.at[kind],
            recv_sem=recv_sems.at[message],
            device_id=device,
            device_id_type=pl.DeviceIdType.MESH,
        )

    to_x = {"seq": x_mate}
    to_y = {"seq": y_mate}
    to_z = {"seq": z_next}
    to_core = {"head": 1 - side}

    def chunk(p):
        return pl.ds(pl.multiple_of(p * part, part), part)

    given = other
    sums = (branch, kept)
    halves = (side, 1 - side)
    pairs = (x, 1 - x)

    steps = [
        (p, pl.ds(first * rows // 16, size * rows // 16)) for p, first, size in STEPS
    ]
    own_copy = [
        local(L_TOKEN + i, tokens_hbm.at[at], own.at[at]) for i, (_, at) in enumerate(steps)
    ]
    gain_copy = local(L_GAIN, gain_hbm, gain)
    freq_copy = local(L_FREQ, freq_hbm, freq)
    post_copy = local(L_POST, post_hbm, post)
    kv_copies = [[], []]
    q_copies = [[], []]
    out_copies = [[], []]
    for i in range(2):
        for f in range(2):
            at_rows = pl.ds(pl.multiple_of(halves[f] * width, width), width)
            for n, source in enumerate((wk_hbm, wv_hbm)):
                columns = pl.ds(pl.multiple_of(pairs[i] * HD, HD), HD)
                kv_copies[i].append(
                    local(
                        L_KV + i,
                        source.at[at_rows, columns],
                        wkv.at[i, pl.ds(f * width, width), pl.ds(n * HD, HD)],
                    )
                )
            columns = pl.ds(pl.multiple_of(pairs[i] * 2 * HD, 2 * HD), 2 * HD)
            q_copies[i].append(
                local(
                    L_Q + i,
                    wq_hbm.at[at_rows, columns],
                    wq.at[i, pl.ds(f * width, width), :],
                )
            )
            at_heads = pl.ds(pl.multiple_of(pairs[i] * 2 * HD, 2 * HD), 2 * HD)
            columns = pl.ds(pl.multiple_of(halves[1 - f] * width, width), width)
            out_copies[i].append(local(L_OUT, wo_hbm.at[at_heads, columns], wo.at[i, f]))

    order = [CHUNKS - 1 - i for i in range(CHUNKS)]
    for c in own_copy[:2]:
        c.start()
    freq_copy.start()
    gain_copy.start()
    for c in kv_copies[0]:
        c.start()
    for c in own_copy[2:]:
        c.start()

    barrier = pltpu.get_barrier_semaphore()

    def greet(device):
        pl.semaphore_signal(barrier, inc=1, device_id=device, device_id_type=pl.DeviceIdType.MESH)

    greet(to_core)
    greet(to_x)
    greet(to_y)
    pl.when(has_next)(lambda: greet(to_z))
    pl.when(has_prev)(lambda: greet({"seq": me - group}))
    pl.semaphore_wait(barrier, 3 + has_next.astype(jnp.int32) + has_prev.astype(jnp.int32))

    def token_copy(i):
        at = steps[i][1]
        return copy(S_TOKEN, TOKEN + i, own.at[at], other.at[at], to_core)

    for i in range(2):
        own_copy[i].wait()
        token_copy(i).start()
    for c in kv_copies[1]:
        c.start()

    def piece(ref, p):
        return ref.at[:, chunk(p), :]

    def of(r):
        return x + r - 2 * x * r

    def send_x(p):
        return copy(S_X, X_KV + p, piece(kvm, p), piece(held.at[0, x], p), to_x)

    def take_x(p):
        return copy(S_X, X_KV + p, piece(kvm, p), piece(held.at[0, 1 - x], p), to_x)

    def place(r, p):
        return r * CHUNKS + CHUNKS - 1 - p

    def move(kind, message, src, dst, b, p, device):
        return copy(kind, message, piece(held.at[src, b], p), piece(held.at[dst, b], p), device)

    def z_near(r, p):
        return move(S_Z_NEAR, Z_NEAR + place(r, p), 0, 2, of(r), p, to_z)

    def z_far(b, p):
        return move(S_Z_FAR, Z_FAR + place(1 - b, p), 2, 4, b, p, to_z)

    def z_extra(p):
        return move(S_Z_FAR, Z_EXTRA + p, 1 + 2 * y, 3 + 2 * y, 0, p, to_z)

    def y_near(src, r, p):
        return move(S_Y_NEAR, Y_NEAR + place(r, p) // (CHUNKS // UNITS), src, 1, of(r), p, to_y)

    def y_far(src, b, p):
        kind = S_Y_FAR if b == 1 else S_Y_LATE
        return move(kind, Y_FAR + place(1 - b, p) // (CHUNKS // UNITS), src, 3, b, p, to_y)

    def y_extra(p):
        return move(S_Y_EXTRA, Y_EXTRA, 3 + 2 * y, 4, 0, p, to_y)

    def rows_of(h):
        return pl.ds(pl.multiple_of(h * unit, unit), unit)

    def take_unit(message, slot, b, h):
        block = held.at[slot, b, :, rows_of(h), :]
        copy(S_Y_NEAR, message, block, block, to_y).wait_recv()

    freq_copy.wait()

    def turn(at):
        at_row = lax.broadcasted_iota(jnp.int32, (at.size, LANES), 0) + (me * rows + at.start)
        angles = at_row.astype(jnp.float32) * freq[...]
        cosine[at, :] = jnp.cos(angles)
        sine[at, :] = jnp.sin(angles)

    turn(pl.ds(order[0] * part, part))
    gain_copy.wait()
    for i in range(2, len(steps)):
        own_copy[i].wait()
        token_copy(i).start()
    for i in (1, 0):
        for c in q_copies[i]:
            c.start()

    lines = 16
    rounds = 4
    tiles = width // LANES

    def norm_chunk(rows_at):
        def step(i, carry):
            start = rows_at.start + i * lines * rounds
            spots = [
                pl.ds(pl.multiple_of(start + n * lines, lines), lines) for n in range(rounds)
            ]
            scales = []
            for at in spots:
                squares = None
                for ref in (own, other):
                    for j in range(tiles):
                        value = ref[at, j * LANES : (j + 1) * LANES].astype(jnp.float32)
                        squares = value * value if squares is None else squares + value * value
                scale = lax.rsqrt(
                    jnp.sum(squares, axis=-1, keepdims=True) / (2 * width) + norm_epsilon
                )
                scales.append(jnp.broadcast_to(scale, (lines, LANES)))
            for f, ref in enumerate((own, other)):
                for j in range(tiles):
                    weight = gain[pl.ds(halves[f] * tiles + j, 1), :]
                    to = f * width + j * LANES
                    for at, scale in zip(spots, scales):
                        value = ref[at, j * LANES : (j + 1) * LANES].astype(jnp.float32)
                        normed[at, to : to + LANES] = (value * scale * weight).astype(jnp.bfloat16)
            return carry

        lax.fori_loop(0, rows_at.size // (lines * rounds), step, 0)

    def project_kv(at, i, dst):
        value = jnp.dot(normed[at, :], wkv[i], preferred_element_type=jnp.float32)
        key = rotated(value[:, :HD], cosine[at, :], sine[at, :])
        dst[0, at, :] = key
        dst[1, at, :] = value[:, HD:].astype(jnp.bfloat16)

    def take_near(r, p):
        def act():
            z_near(r, p).wait_recv()
            pl.when(second_row)(lambda: y_near(2, r, p).start())

        pl.when(has_prev)(act)

    far_order = [(1, 3), (1, 2), (1, 1), (1, 0), (0, 3), (0, 2)]
    late_order = [(0, 1), (0, 0), (1, 1), (1, 0), (0, 3), (0, 2)]

    def take_far(k):
        b, p = far_order[k]

        def act():
            z_far(b, p).wait_recv()
            pl.when(second_row)(lambda: y_far(4, b, p).start())

        pl.when(has_far)(act)

    def take_extra(p):
        def act():
            z_extra(p).wait_recv()
            y_extra(p).start()

        pl.when(has_far)(act)

    def pass_extra(row):
        def act():
            for p in (1, 0):
                z_extra(p).start()

        pl.when(has_next & has_prev & (y == row))(act)

    def pass_mate(p):
        take_x(p).wait_recv()
        pl.when(has_next)(lambda: z_near(1, p).start())
        pl.when(first_row)(lambda: y_near(0, 1, p).start())

    def rows_copy(kind, message, src, dst, at, device):
        copy(kind, message, src.at[:, at, :], dst.at[:, at, :], device).start()

    for i, (p, at) in enumerate(steps):
        token_copy(i).wait_recv()
        norm_chunk(at)
        if i > 1:
            turn(at)
        if i == 0:
            local(L_KV, wkv.at[0], wkv.at[0]).wait()
        project_kv(at, 0, held.at[0, x])

        def near_rows(slot, kind, message, device):
            rows_copy(kind, message, held.at[0, x], held.at[slot, x], at, device)

        pl.when(has_next)(lambda: near_rows(2, S_Z_NEAR, Z_NEAR + place(0, p), to_z))
        pl.when(first_row)(
            lambda: near_rows(1, S_Y_NEAR, Y_NEAR + place(0, p) // (CHUNKS // UNITS), to_y)
        )
        if i == 0:
            continue
        if i == 4:
            take_near(0, order[1])
        if i == 1:
            local(L_KV + 1, wkv.at[1], wkv.at[1]).wait()
            for c in out_copies[0] + out_copies[1]:
                c.start()
            post_copy.start()
        project_kv(pl.ds(p * part, part), 1, kvm)
        send_x(p).start()
        if i == 2:
            take_near(0, order[0])

    def project_q(i, dst):
        def step(t, carry):
            at = pl.ds(pl.multiple_of(t * unit, unit), unit)
            value = jnp.dot(normed[at, :], wq[i], preferred_element_type=jnp.float32)
            for head in range(2):
                dst[pl.ds(pl.multiple_of(head * rows + t * unit, unit), unit), :] = rotated(
                    value[:, head * HD : (head + 1) * HD], cosine[at, :], sine[at, :]
                )
            return carry

        lax.fori_loop(0, UNITS, step, 0)

    def q_copy():
        return copy(S_Q, X_Q, asked, queries.at[1], to_x)

    total[...] = jnp.zeros_like(total)
    mass[...] = jnp.zeros_like(mass)
    pass_mate(order[0])
    local(L_Q + 1, wq.at[1], wq.at[1]).wait()
    project_q(1, asked)
    q_copy().start()
    pass_mate(order[1])
    take_near(0, order[2])
    local(L_Q + 0, wq.at[0], wq.at[0]).wait()
    project_q(0, queries.at[0])
    pass_mate(order[2])
    take_near(0, order[3])
    pass_mate(order[3])

    def attend(which, slot, b, h, distance=None):
        at = pl.ds(pl.multiple_of(h * unit, unit), unit)
        scores = lax.dot_general(
            queries[which],
            held[slot, b, 0, at, :],
            (((1,), (1,)), ((), ())),
            preferred_element_type=jnp.float32,
        )
        weights = jnp.exp2(outer * jnp.tanh(scores * inner))
        if distance is not None:
            down = lax.broadcasted_iota(jnp.int32, weights.shape, 0)
            down = jnp.where(down >= rows, down - rows, down)
            offset = (distance - h * unit) + down - lax.broadcasted_iota(jnp.int32, weights.shape, 1)
            weights = jnp.where((offset >= 0) & (offset < WINDOW), weights, 0.0)
        added = None
        for k in range(unit // LANES):
            lanes = weights[:, k * LANES : (k + 1) * LANES]
            added = lanes if added is None else added + lanes
        mass[which] += added
        total[which] += jnp.dot(
            weights.astype(jnp.bfloat16), held[slot, b, 1, at, :], preferred_element_type=jnp.float32
        )

    def both(act):
        def step(s, carry):
            act(s)
            return carry

        lax.fori_loop(0, 2, step, 0)

    def attend_own(which):
        mine = of(which)

        def step(i, carry):
            b = mine - i // UNITS
            if which == 1:
                pl.when(i == 1)(lambda: take_far(0))
            attend(which, 0, b, i % UNITS, (mine - b) * rows)
            return carry

        lax.fori_loop(0, UNITS + UNITS * mine, step, 0)

    def z_unit(u):
        return 2, of(u // UNITS), UNITS - 1 - u % UNITS

    def y_unit(w):
        return 1, of(w // UNITS), UNITS - 1 - w % UNITS

    near_there = me >= 2
    far_there = me >= 6

    def take_y(w):
        take_unit(Y_NEAR + w, *y_unit(w))

    def near_pass(u):
        p = CHUNKS - 1 - u
        take_near(1, p)
        pl.when(has_prev & has_next)(lambda: z_far(1, p).start())
        pl.when(has_prev & first_row & (u < 2))(lambda: y_far(2, 1, p).start())

    near_pass(0)
    attend_own(0)

    def near_step(u, carry):
        pl.when(u >= 1)(lambda: near_pass(u))
        pl.when(has_prev)(lambda: attend(0, *z_unit(u)))

        def with_y():
            take_y(u - 1)
            attend(0, *y_unit(u - 1))

        pl.when((u >= 1) & near_there)(with_y)
        return carry

    lax.fori_loop(0, CHUNKS, near_step, 0)

    def pass_rest():
        for p in (3, 2):
            pl.when(has_next)(lambda: z_far(0, p).start())
        for b, p in late_order:
            pl.when(first_row)(lambda: y_far(2, b, p).start())

    pl.when(has_prev)(pass_rest)

    q_copy().wait_recv()
    attend_own(1)

    def again_z(u, carry):
        pl.when(u == 1)(lambda: take_far(1))
        attend(1, *z_unit(u))
        return carry

    def again_y(w, carry):
        pl.when(w == 2)(lambda: take_far(2))
        attend(1, *y_unit(w))
        return carry

    def repeat(count, step):
        def act():
            lax.fori_loop(0, count, step, 0)

        return act

    pl.when(has_prev)(repeat(4, again_z))
    pl.when(near_there)(repeat(3, again_y))

    def last_near():
        take_y(3)
        both(lambda s: attend(s, *y_unit(3)))

    pl.when(near_there)(last_near)
    pass_extra(0)

    third_b = (1, 1 - y, y, 0)
    third_h = (1, 0, 1 - y, y)

    def take_third(j):
        def act():
            message = Y_FAR + 2 * (1 - third_b[j]) + 1 - third_h[j]
            take_unit(message, 3, third_b[j], third_h[j])

        pl.when(far_there & ((j < 3) | second_row))(act)

    def third(j):
        pl.when(far_there)(lambda: both(lambda s: attend(s, 3, third_b[j], third_h[j])))

    def fourth(b, h):
        def act():
            def one(s):
                mine = of(s)
                pl.when(mine <= b)(lambda: attend(s, 4, b, h, WINDOW + (mine - b) * rows))

            both(one)

        pl.when(has_far)(act)

    take_far(3)
    fourth(1, 1)
    take_third(0)
    third(0)
    take_far(4)
    fourth(1, 0)
    pl.when(second_row)(lambda: take_third(1))
    pass_extra(1)
    pl.when(first_row)(lambda: take_third(1))
    third(1)
    take_far(5)
    fourth(0, 1)
    pl.when(second_row)(lambda: take_third(2))
    pl.when(second_row)(lambda: third(2))
    take_extra(1)
    pl.when(first_row)(lambda: take_third(2))

    def late(which):
        attend(which, 3, third_b[2], third_h[2])

    pl.when(far_there & first_row)(lambda: late(1))
    take_extra(0)
    take_third(3)
    pl.when(far_there)(lambda: attend(1, 3, third_b[3], third_h[3]))

    def slab(p):
        first, size = SLABS[p]
        return pl.ds(first * rows // 16, size * rows // 16)

    def finish(which, head, at_rows):
        at = pl.ds(head * rows + at_rows.start, at_rows.size)
        weight = jnp.sum(mass[which, at, :], axis=-1, keepdims=True)
        return (total[which, at, :] * (1.0 / weight)).astype(jnp.bfloat16)

    def out_copy(p):
        return copy(S_OUT, X_OUT + p, leaving.at[slab(p)], landed.at[slab(p)], to_x)

    def send_out(p):
        for head in range(2):
            leaving[slab(p), head * HD : (head + 1) * HD] = finish(1, head, slab(p))
        out_copy(p).start()

    def project_own(h):
        at = slice(h * unit, (h + 1) * unit)
        for p in (range(2) if h else range(2, OUTS)):
            for head in range(2):
                finished[slab(p), head * HD : (head + 1) * HD] = finish(0, head, slab(p))
        for f in range(2):
            sums[f][at, :] = jnp.dot(
                finished[at, :], wo[0, f], preferred_element_type=jnp.float32
            )

    def send_low():
        for p in range(2, OUTS):
            send_out(p)

    def send_high():
        for p in range(2):
            send_out(p)

    send_high()
    pl.when(x == 0)(send_low)
    pl.when(far_there & first_row)(lambda: late(0))
    pl.when(far_there)(lambda: attend(0, 3, third_b[3], third_h[3]))
    local(L_OUT, wo, wo).wait()
    post_copy.wait()
    project_own(1)

    def last_far():
        take_unit(Y_EXTRA, 4, 0, 0)
        attend(x, 4, 0, 0, WINDOW)

    pl.when(has_far)(last_far)
    pl.when(x == 1)(send_low)
    project_own(0)

    def given_copy(p):
        return copy(S_GIVEN, GIVEN + p, given.at[slab(p)], arrived.at[slab(p)], to_core)

    def squares_copy(p):
        return copy(S_SQUARES, SQUARES + p, sq_own.at[slab(p)], sq_other.at[slab(p)], to_core)

    def give(p):
        out_copy(p).wait_recv()
        given[slab(p), :] = (
            branch[slab(p), :]
            + jnp.dot(landed[slab(p), :], wo[1, 0], preferred_element_type=jnp.float32)
        ).astype(jnp.bfloat16)
        given_copy(p).start()

    def keep(p):
        kept[slab(p), :] += jnp.dot(
            landed[slab(p), :], wo[1, 1], preferred_element_type=jnp.float32
        )

    def groups(p):
        return [pl.ds(slab(p).start + n * lines, lines) for n in range(slab(p).size // lines)]

    columns = [slice(j * LANES, (j + 1) * LANES) for j in range(tiles)]

    def add_core(p):
        given_copy(p).wait_recv()
        for rows_at in groups(p):
            shares = [kept[rows_at, at] + arrived[rows_at, at].astype(jnp.float32) for at in columns]
            squares = None
            for at, share in zip(columns, shares):
                kept[rows_at, at] = share
                squares = share * share if squares is None else squares + share * share
            sq_own[rows_at, :] = squares
        squares_copy(p).start()

    def last(p):
        squares_copy(p).wait_recv()
        for rows_at in groups(p):
            squares = jnp.sum(sq_own[rows_at, :] + sq_other[rows_at, :], axis=-1, keepdims=True)
            scale = jnp.broadcast_to(
                lax.rsqrt(squares / (2 * width) + norm_epsilon), (lines, LANES)
            )
            values = [
                own[rows_at, at].astype(jnp.float32) + post[j : j + 1, :] * kept[rows_at, at] * scale
                for j, at in enumerate(columns)
            ]
            for at, value in zip(columns, values):
                out_ref[rows_at, at] = value.astype(jnp.bfloat16)

    for p in range(OUTS - 2):
        give(p)
        keep(p)
        if p >= 1:
            add_core(p - 1)
        if p >= 2:
            last(p - 2)
    give(OUTS - 2)
    give(OUTS - 1)
    keep(OUTS - 2)
    keep(OUTS - 1)
    for p in range(OUTS - 3, OUTS):
        add_core(p)
    for p in range(OUTS - 4, OUTS):
        last(p)

    def sent(kind, ref):
        copy(kind, TOKEN, ref, ref, to_x).wait_send()

    block = held.at[0, 0]
    sent(S_TOKEN, own)
    sent(S_X, kvm)
    sent(S_Q, asked)
    sent(S_OUT, leaving)
    sent(S_GIVEN, given)
    sent(S_SQUARES, sq_own)
    pl.when(has_next)(lambda: sent(S_Z_NEAR, held.at[0]))
    pl.when(has_next & has_prev)(lambda: sent(S_Z_FAR, held.at[0]))
    pl.when(first_row | has_prev)(lambda: sent(S_Y_NEAR, held.at[0]))
    pl.when((first_row & has_prev) | has_far)(lambda: sent(S_Y_FAR, block))
    pl.when(first_row & has_prev)(lambda: sent(S_Y_LATE, block))
    pl.when(second_row & has_far)(lambda: sent(S_Y_LATE, block.at[:, rows_of(0), :]))
    pl.when(has_far)(lambda: sent(S_Y_EXTRA, block.at[:, rows_of(0), :]))


def local_layer(blocks, tokens, pre_gain, query_weight, key_weight, value_weight, out_weight, post_gain):
    rows, width = tokens.shape
    frequency = np.exp(-np.log(rope_base) * (2.0 * np.arange(HD // 2) / HD)).astype(np.float32)
    anywhere = pl.BlockSpec(memory_space=pltpu.HBM)
    bf16, f32 = jnp.bfloat16, jnp.float32
    vmem = pltpu.VMEM
    half = 2 * HD
    normed_branch = pl.pallas_call(
        functools.partial(layer_kernel, blocks),
        out_shape=vmem((rows, width), bf16),
        in_specs=[anywhere] * 8,
        out_specs=pl.BlockSpec(memory_space=pltpu.VMEM),
        scratch_shapes=[
            vmem((rows, width), bf16),
            vmem((rows, width), bf16),
            vmem((2 * width // LANES, LANES), f32),
            vmem((1, LANES), f32),
            vmem((width // LANES, LANES), f32),
            vmem((rows, 2 * width), bf16),
            vmem((2, 2 * width, half), bf16),
            vmem((2, 2 * width, half), bf16),
            vmem((2, 2, half, width), bf16),
            vmem((rows, LANES), f32),
            vmem((rows, LANES), f32),
            vmem((6, 2, 2, rows, HD), bf16),
            vmem((2, rows, HD), bf16),
            vmem((2, 2 * rows, HD), bf16),
            vmem((2 * rows, HD), bf16),
            vmem((2, 2 * rows, HD), f32),
            vmem((2, 2 * rows, LANES), f32),
            vmem((rows, half), bf16),
            vmem((rows, half), bf16),
            vmem((rows, half), bf16),
            vmem((rows, width), f32),
            vmem((rows, width), f32),
            vmem((rows, width), bf16),
            vmem((rows, LANES), f32),
            vmem((rows, LANES), f32),
            pltpu.SemaphoreType.DMA((SENDS,)),
            pltpu.SemaphoreType.DMA((MESSAGES,)),
            pltpu.SemaphoreType.DMA((LOCALS,)),
        ],
        compiler_params=pltpu.CompilerParams(
            collective_id=0, has_side_effects=True, vmem_limit_bytes=58 * 1024 * 1024
        ),
    )(
        tokens,
        pre_gain.reshape(-1, LANES),
        jnp.asarray(frequency)[None, :],
        query_weight,
        key_weight,
        value_weight,
        out_weight,
        post_gain.reshape(-1, LANES),
    )
    return normed_branch


def solution(mesh):
    placed = (
        P("seq", "head"),
        P(),
        P(None, "head"),
        P(None, "head"),
        P(None, "head"),
        P("head", None),
        P("head"),
    )
    return jax.shard_map(
        functools.partial(local_layer, mesh.shape["seq"]),
        mesh=mesh,
        in_specs=placed,
        out_specs=P("seq", "head"),
        check_vma=False,
    )
```
